32 devices in a mesh: dp: 8 (over y, x, core), seq: 4 (over z).
Axes of the slice: x: 2, y: 2, z: 4, core: 2. Of those that a mesh axis runs over, the one named last changes fastest.
Arguments:
- student_in: bfloat16 [4096, 3584], P(('dp', 'seq')), may hold values from -6 to 6
- weight: bfloat16 [3584, 512], P(('dp', 'seq')), may hold values from -0.09375 to 0.09375
- queries: bfloat16 [4096, 512], P(('dp', 'seq')), may hold values from -8 to 8, as said below
- keys: bfloat16 [4096, 128], P(('dp', 'seq')), may hold values from -8 to 8
- values: bfloat16 [4096, 128], P(('dp', 'seq')), may hold values from -6 to 6
- lengths: int32 [8, 4], P('dp'), may hold values from 1 to 384, 512 in all within a row
- assignment: int32 [8, 4], P('dp'), may hold values from 0 to 3, each once within a row
Outputs:
- attention: bfloat16 [4096, 512], P(('dp', 'seq'))
- weight_grad: float32 [3584, 512], P(('dp', 'seq'))
The draws below stay inside these ranges and needn't reach their ends.
Inputs may be any that keep to these rules, and one draw needn't show every extreme that they name: `queries`: entries of head 0 and of keys may reach the ends of this range. Each row holds the lengths of 4 rollouts of one sequence, summing to 512, the longest exactly 384. `assignment`: each row is a permutation of the 4 rollout blocks of one sequence.
All inputs are finite; a program needn't handle non-finite values.
Results may differ from the reference program's by a relative error of at most 0.012.
Values may be sent and summed in bfloat16 or wider, within the bound.
A program may use at most 64 MiB of HBM per device.

```python
import math
import jax
import jax.numpy as jnp
import numpy as np
from jax import lax

HD = 128
HQ = 4
DS = 3584
BLK = 128
DOCS = 4
SEQLEN = 512
TOKENS_ALL = 4096
NBLK = 4
MAXLEN = 384
N_DP = 8


def draw_queries(key, part):
    noise_key = jax.random.fold_in(key, 11)
    drawn = jnp.clip(jax.random.normal(noise_key, (TOKENS_ALL, HQ * HD), jnp.float32), -8.0, 8.0)
    return drawn.astype(jnp.bfloat16)


def draw_keys(key, part):
    noise_key = jax.random.fold_in(key, 13)
    drawn = jnp.clip(jax.random.normal(noise_key, (TOKENS_ALL, HD), jnp.float32), -8.0, 8.0)
    return drawn.astype(jnp.bfloat16)


def with_spikes(values, key, source, target, blocks, factor):
    def block_of(axis_at):
        return (jnp.arange(values.shape[axis_at]) // (values.shape[axis_at] // blocks)).reshape((-1,) + (1,) * (values.ndim - 1 - axis_at))

    first = jax.random.permutation(key, blocks)[block_of(target)]
    far = (block_of(target) + blocks // 2) % blocks
    return jnp.where((block_of(source) == first) | (block_of(source) == far), factor * values, values)


def block_scale(rng, dims, split, least, largest):
    gain = 1.0
    for dim, blocks in split:
        steps = jax.random.uniform(jax.random.fold_in(jax.random.fold_in(rng, 6), dim), (blocks,), jnp.float32, least / len(split), largest / len(split))
        gain = gain * jnp.repeat(jnp.exp(steps), dims[dim] // blocks).reshape((-1,) + (1,) * (len(dims) - 1 - dim))
    return gain


def split_up(amount, total, limit, lean):
    weights = [(1 << 20) // math.isqrt(grade ** lean) + 1 for grade in range(2, amount + 1)]
    rest, holding = total - limit - (amount - 1), [1] * (amount - 1)
    while rest > 0:
        candidates = [i for i in range(amount - 1) if holding[i] < limit]
        mass, left = sum([weights[i] for i in candidates]), rest
        for i in candidates:
            extra = min(limit - holding[i], max(1, left * weights[i] // mass), rest)
            holding[i] = holding[i] + extra
            rest = rest - extra
    return np.array([limit] + holding)


def uneven_parts(own_key, count, total, bound, lean):
    if count == 2:
        one = jax.random.randint(own_key, (), max(1, total - bound), min(bound, total - 1) + 1)
        return jnp.stack([one, total - one])
    sizes = jnp.asarray(split_up(count, total, bound, lean), jnp.int32)
    pairs = (count - 1) // 2
    donor, taker = sizes[1:1 + 2 * pairs:2], sizes[2:2 + 2 * pairs:2]
    slack = jnp.minimum(donor - 1, bound - taker)
    moved = jax.random.randint(jax.random.fold_in(own_key, 1), (pairs,), 0, 1 << 20) % (slack + 1)
    sizes = sizes.at[1:1 + 2 * pairs:2].set(donor - moved).at[2:2 + 2 * pairs:2].set(taker + moved)
    return sizes[jax.random.permutation(jax.random.fold_in(own_key, 2), count)]


def scatter_about(own_key, extent, scale, reach, cuts=(), kind=jnp.bfloat16):
    result = scale * jax.random.normal(own_key, extent, jnp.float32)
    if cuts:
        result = result * block_scale(own_key, extent, cuts, -0.22, 0.18)
    return jnp.clip(result, -reach, reach).astype(kind)


def bell_draw_with(own_key, shape, width, most, shards, heavy, kind=jnp.bfloat16):
    values = width * jax.random.normal(own_key, shape, jnp.float32)
    if shards:
        values = values * block_scale(own_key, shape, shards, -0.22, 0.18)
    return jnp.clip(with_spikes(values, jax.random.fold_in(own_key, 3), *heavy), -most, most).astype(kind)


def setup_inputs(seed: int = 0) -> dict:
    arg_keys = jax.random.split(jax.random.key(seed), 8)
    student_in = bell_draw_with(arg_keys[0], (TOKENS_ALL, DS), 1.0, 6.0, ((0, 32),), (0, 1, 32, 2.75))
    weight = scatter_about(arg_keys[1], (DS, HQ * HD), DS ** -0.5, 0.09375, ((0, 32),))
    queries = draw_queries(jax.random.fold_in(arg_keys[7], 71), 0)
    keys = draw_keys(jax.random.fold_in(arg_keys[7], 71), 0)
    values = scatter_about(arg_keys[4], (TOKENS_ALL, HD), 1.0, 6.0, ((0, 32),))
    lengths = jax.vmap(lambda own: uneven_parts(own, DOCS, SEQLEN, MAXLEN, 2))(jax.random.split(arg_keys[5], N_DP)).reshape((N_DP, DOCS)).astype(jnp.int32)
    assignment = jax.vmap(lambda own: jax.random.permutation(own, NBLK))(jax.random.split(arg_keys[6], N_DP)).reshape((N_DP, NBLK)).astype(jnp.int32)
    return {"student_in": student_in, "weight": weight, "queries": queries, "keys": keys, "values": values, "lengths": lengths, "assignment": assignment}


EPSILON = 1e-06
NEGATIVE = -1e+30

def locate(assign_row, length_row):
    slot_ids = jnp.arange(SEQLEN, dtype=jnp.int32)
    position = (assign_row[slot_ids // BLK] * BLK + slot_ids % BLK).astype(jnp.int32)
    doc_ends = jnp.cumsum(length_row).astype(jnp.int32)
    document = lax.optimization_barrier(jnp.sum((position[:, None] >= doc_ends[None, :]).astype(jnp.int32), axis=1))
    return (position, document)

def attend(query_rows, key_rows, value_rows, position, document):
    step_rows = math.gcd(SEQLEN, 512)
    blocks = query_rows.reshape(SEQLEN // step_rows, step_rows, HQ, HD)

    def one_block(block_items):
        query_block, query_pos, query_doc = block_items
        scores = jnp.einsum('qhd,kd->hqk', query_block.astype(jnp.float32), key_rows.astype(jnp.float32)) * HD ** (-0.5)
        allowed = (query_doc[:, None] == document[None, :]) & (query_pos[:, None] >= position[None, :])
        masked = jnp.where(allowed[None], scores, NEGATIVE)
        row_top = lax.optimization_barrier(jnp.max(masked, axis=-1, keepdims=True))
        exp_terms = jnp.where(allowed[None], jnp.exp(masked - row_top), 0.0)
        totals = lax.optimization_barrier(jnp.sum(exp_terms, axis=-1))
        rounded = lax.optimization_barrier(exp_terms.astype(jnp.bfloat16)).astype(jnp.float32)
        mixture = jnp.einsum('hqk,kd->qhd', rounded, value_rows.astype(jnp.float32))
        return (mixture / totals.T[:, :, None]).astype(jnp.bfloat16)
    attended = lax.map(one_block, (blocks, position.reshape(-1, step_rows), document.reshape(-1, step_rows)))
    return attended.reshape(SEQLEN, HQ * HD)

def reference(student_in, weight, queries, keys, values, lengths, assignment):

    def sequence(running, per_seq):
        rows_in, query_rows, key_rows, value_rows, length_row, assign_row = per_seq
        position, document = locate(assign_row, length_row)
        attended = attend(query_rows, key_rows, value_rows, position, document)
        as_float = rows_in.astype(jnp.float32)
        normed = (as_float * lax.rsqrt(lax.optimization_barrier(jnp.mean(as_float * as_float, axis=1, keepdims=True)) + EPSILON)).astype(jnp.bfloat16)
        predicted = jnp.dot(normed, weight, preferred_element_type=jnp.float32)
        scaled = ((predicted - attended.astype(jnp.float32)) * TOKENS_ALL ** (-0.5)).astype(jnp.bfloat16)
        partial_sum = lax.dot_general(normed, scaled, (((0,), (0,)), ((), ())), preferred_element_type=jnp.float32)
        return (running + partial_sum, attended)
    stacked = (student_in.reshape(N_DP, SEQLEN, DS), queries.reshape(N_DP, SEQLEN, HQ * HD), keys.reshape(N_DP, SEQLEN, HD), values.reshape(N_DP, SEQLEN, HD), lengths, assignment)
    weight_grad, attention = lax.scan(sequence, jnp.zeros((DS, HQ * HD), jnp.float32), stacked)
    return (attention.reshape(TOKENS_ALL, HQ * HD), weight_grad)
```

```python
import functools
import math

import jax
import jax.numpy as jnp
from jax import lax
from jax.experimental import pallas as pl
from jax.experimental.pallas import tpu as pltpu
from jax.sharding import PartitionSpec as P

HD = 128
HQ = 4
BLK = 128


EPSILON = 1e-06
NEGATIVE = -1e30


def locate(assign_row, doc_ends, first_slot, count):
    slot_ids = first_slot + jnp.arange(count, dtype=jnp.int32)
    block_ids = slot_ids // BLK
    block_table = jnp.arange(assign_row.shape[0], dtype=jnp.int32)
    placed = jnp.sum(
        jnp.where(block_ids[:, None] == block_table[None, :], assign_row[None, :], 0), axis=1
    )
    position = placed * BLK + slot_ids % BLK
    document = jnp.sum((position[:, None] >= doc_ends[None, :]).astype(jnp.int32), axis=1)
    return (position, document)


def absorb_block(state, key_block, value_block, query_heads, allowed):
    run_max, run_total, run_acc = state
    scores = jnp.einsum(
        "qhd,kd->hqk", query_heads, key_block, preferred_element_type=jnp.float32
    ) * HD ** (-0.5)
    masked = jnp.where(allowed[None], scores, NEGATIVE)
    new_max = jnp.maximum(run_max, jnp.max(masked, axis=-1))
    fading = jnp.exp(run_max - new_max)
    exp_terms = jnp.where(allowed[None], jnp.exp(masked - new_max[:, :, None]), 0.0)
    new_total = run_total * fading + jnp.sum(exp_terms, axis=-1)
    mixture = jnp.einsum(
        "hqk,kd->qhd",
        exp_terms.astype(jnp.bfloat16),
        value_block,
        preferred_element_type=jnp.float32,
    )
    new_acc = run_acc * fading.T[:, :, None] + mixture
    return (new_max, new_total, new_acc)


def local(student_in, weight, queries, keys, values, lengths, assignment):
    rows = queries.shape[0]
    assign_row = assignment[0]
    doc_ends = jnp.cumsum(lengths[0])
    query_pos, query_doc = locate(assign_row, doc_ends, lax.axis_index("seq") * rows, rows)
    query_heads = queries.reshape(rows, HQ, HD)
    start_state = (
        jnp.full((HQ, rows), NEGATIVE, jnp.float32),
        jnp.zeros((HQ, rows), jnp.float32),
        jnp.zeros((rows, HQ, HD), jnp.float32),
    )
    key_piece = lax.all_gather(keys, "seq", axis=0, tiled=True)
    value_piece = lax.all_gather(values, "seq", axis=0, tiled=True)
    count = key_piece.shape[0]
    step_rows = math.gcd(count, 512)
    steps_count = count // step_rows
    key_pos, key_doc = locate(assign_row, doc_ends, jnp.int32(0), count)

    def one_step(running, slabs):
        key_block, value_block, key_position, key_document = slabs
        allowed = (query_doc[:, None] == key_document[None, :]) & (
            query_pos[:, None] >= key_position[None, :]
        )
        updated = absorb_block(running, key_block, value_block, query_heads, allowed)
        return (updated, None)

    slabs = (
        key_piece.reshape(steps_count, step_rows, HD),
        value_piece.reshape(steps_count, step_rows, HD),
        key_pos.reshape(steps_count, step_rows),
        key_doc.reshape(steps_count, step_rows),
    )
    result, _ = lax.scan(one_step, start_state, slabs)
    final_max, final_total, final_acc = result
    attention = (final_acc / final_total.T[:, :, None]).reshape(rows, HQ * HD).astype(jnp.bfloat16)
    as_float = student_in.astype(jnp.float32)
    normed = (
        as_float * lax.rsqrt(jnp.mean(as_float * as_float, axis=1, keepdims=True) + EPSILON)
    ).astype(jnp.bfloat16)
    group_rows = lax.all_gather(weight, "seq", axis=0, tiled=True)
    columns = normed
    predicted = jnp.dot(
        columns,
        lax.all_gather(group_rows, "dp", axis=0, tiled=True),
        preferred_element_type=jnp.float32,
    )
    dp_count = lax.axis_size("dp")
    seq_count = lax.axis_size("seq")
    token_total = rows * dp_count * seq_count
    scaled = ((predicted - attention.astype(jnp.float32)) * token_total ** (-0.5)).astype(
        jnp.bfloat16
    )
    columns = normed
    outer_rows = lax.psum_scatter(
        lax.dot_general(
            columns, scaled, (((0,), (0,)), ((), ())), preferred_element_type=jnp.float32
        ).astype(jnp.bfloat16),
        "dp",
        scatter_dimension=0,
        tiled=True,
    )
    weight_grad = lax.psum_scatter(outer_rows, "seq", scatter_dimension=0, tiled=True).astype(
        jnp.float32
    )
    return (attention, weight_grad)


MESH = pl.DeviceIdType.MESH
F32 = jnp.float32
BF16 = jnp.bfloat16


def fused_kernel(
    token_total,
    x_ref, w_ref, q_ref, k_ref, v_ref, len_ref, asg_ref,
    att_ref, out_ref,
    xs, xt, w_all, kv_all, inv, pred, p_out, p_in, s_all, att_half, att_peer,
    grad_f, s_y, r_y, s_z, r_z,
    send, send_z, sem_w, sem_kv, sem_x, sem_inv, sem_att, sem_p, sem_s, sem_ry, sem_rz,
):
    rows = q_ref.shape[0]
    piece = w_ref.shape[0]
    half = w_ref.shape[1] // 2
    chunk = half // 2
    depth = xs.shape[3]
    dp, z = lax.axis_index("dp"), lax.axis_index("seq")
    c = dp % 2
    pc = 1 - c
    x = (dp // 2) % 2
    y = dp // 4
    yo = 1 - y
    dp_m = dp + 1 - 2 * c
    mate = (dp_m, z)
    xn_dev = (dp + 2 - 4 * x, z)
    yn_dev = (dp + 4 - 8 * y, z)
    yn_mate = (dp_m + 4 - 8 * y, z)
    zs = (z, z + 1 - 2 * (z % 2), z + 2 - 4 * (z // 2), 3 - z)
    z_dev = [(dp, zs[r]) for r in range(4)]
    z_mate = [(dp_m, zs[r]) for r in range(4)]
    below, above = (dp, (z + 3) % 4), (dp, (z + 1) % 4)
    below_m, above_m = (dp_m, (z + 3) % 4), (dp_m, (z + 1) % 4)

    barrier = pltpu.get_barrier_semaphore()
    for dev in (mate, xn_dev, yn_dev, yn_mate):
        pl.semaphore_signal(barrier, inc=1, device_id=dev, device_id_type=MESH)
    for present, pair in ((z > 0, (below, below_m)), (z < 3, (above, above_m))):

        @pl.when(present)
        def _():
            for dev in pair:
                pl.semaphore_signal(barrier, inc=1, device_id=dev, device_id_type=MESH)

    pl.semaphore_wait(barrier, 4 + 2 * (jnp.minimum(z, 1) + jnp.minimum(3 - z, 1)))

    sent = []
    sent_when = []

    def push_when(present, src, dst, rsem, dev):
        copy = pltpu.make_async_remote_copy(
            src_ref=src, dst_ref=dst, send_sem=send_z.at[len(sent_when)], recv_sem=rsem,
            device_id=dev, device_id_type=MESH,
        )
        pl.when(present)(copy.start)
        sent_when.append((present, copy))

    def both_ways(src, dst, rsem, down, up):
        push_when(z > 0, src, dst, rsem, down)
        push_when(z < 3, src, dst, rsem, up)

    def push(src, dst, rsem, dev):
        copy = pltpu.make_async_remote_copy(
            src_ref=src, dst_ref=dst, send_sem=send.at[len(sent)], recv_sem=rsem,
            device_id=dev, device_id_type=MESH,
        )
        copy.start()
        sent.append(copy)

    def arrive(dst, rsem):
        pltpu.make_async_remote_copy(
            src_ref=dst, dst_ref=dst, send_sem=send.at[0], recv_sem=rsem,
            device_id=mate, device_id_type=MESH,
        ).wait_recv()

    def cols(core, j):
        return pl.ds(pl.multiple_of(core * half + j * chunk, 128), chunk)

    def width(at_y, at_x):
        return pl.ds(pl.multiple_of((at_y * 2 + at_x) * depth, 128), depth)

    def w_arrive(at):
        arrive(w_all.at[at], sem_w.at[at])

    def x_push(at_y, at_x, slot, dev):
        push(x_ref.at[:, width(at_y, at_x)], xs.at[at_y, slot], sem_x.at[at_y, slot], dev)

    def w_start(j):
        at = (j, y, c, z)
        dst, sem = w_all.at[at], sem_w.at[at]
        own, peer = w_ref.at[:, cols(c, j)], w_ref.at[:, cols(pc, j)]
        both_ways(own, dst, sem, below, above)
        push(own, dst, sem, yn_dev)
        both_ways(peer, dst, sem, below_m, above_m)
        push(peer, dst, sem, yn_mate)
        push(peer, dst, sem, mate)

    w_start(0)
    x_push(y, 1 - x, 2, xn_dev)
    x_push(yo, 1 - x, 2, xn_dev)
    w_start(1)
    both_ways(k_ref, kv_all.at[0, z], sem_kv.at[0, z], below, above)
    both_ways(v_ref, kv_all.at[1, z], sem_kv.at[1, z], below, above)
    x_push(y, x, 1, mate)
    x_push(yo, x, 1, mate)
    for j in range(2):
        w_all[j, y, c, z] = w_ref[:, cols(c, j)]
    kv_all[0, z] = k_ref[...]
    kv_all[1, z] = v_ref[...]
    xs[y, 0] = x_ref[:, width(y, x)]
    xs[yo, 0] = x_ref[:, width(yo, x)]

    step = 16

    @pl.loop(0, rows // step)
    def _(i):
        at = pl.ds(pl.multiple_of(i * step, step), step)
        block = x_ref[at, :].astype(F32)
        factor = lax.rsqrt(jnp.mean(block * block, axis=1, keepdims=True) + EPSILON)
        inv[0, at, :] = jnp.broadcast_to(factor, (step, 128))

    push(inv.at[0], inv.at[1], sem_inv.at[0], mate)

    def sources(k):
        return (
            (z >= k, (z >= k) & (z < 3), (z + 4 - k) % 4, above),
            (z + k <= 3, (z + k <= 3) & (z > 0), (z + k) % 4, below),
        )

    def forward(j, k):
        for part in range(2):
            for present, onward, at_z, dev in sources(k):
                at = (j, y, part, at_z)

                @pl.when(present)
                def _():
                    w_arrive(at)

                if k < 3:
                    push_when(onward, w_all.at[at], w_all.at[at], sem_w.at[at], dev)
                push_when(present, w_all.at[at], w_all.at[at], sem_w.at[at], yn_dev)

    def kv_forward(k):
        for part in range(2):
            for present, onward, at_z, dev in sources(k):
                at = (part, at_z)

                @pl.when(present)
                def _():
                    arrive(kv_all.at[at], sem_kv.at[at])

                if k < 3:
                    push_when(onward, kv_all.at[at], kv_all.at[at], sem_kv.at[at], dev)

    def x_arrive(at_y, slot):
        arrive(xs.at[at_y, slot], sem_x.at[at_y, slot])

    def x_relay(at_y):
        x_arrive(at_y, 2)
        push(xs.at[at_y, 2], xs.at[at_y, 3], sem_x.at[at_y, 3], mate)

    def turn(at_y, slot):
        for j in range(depth // 128):
            at = slice(j * 128, (j + 1) * 128)
            xt[at_y, at, slot * rows : (slot + 1) * rows] = xs[at_y, slot, :, at].T

    def product(j, at_y, first):
        return jnp.dot(
            xs[at_y, first : first + 2].reshape(2 * rows, depth),
            w_all[j, at_y].reshape(depth, chunk),
            preferred_element_type=F32,
        )

    forward(0, 1)
    forward(1, 1)
    kv_forward(1)
    x_arrive(y, 1)
    x_arrive(yo, 1)
    for slot in range(2):

        @pl.loop(0, 2)
        def _(at_y):
            turn(at_y, slot)

    forward(0, 2)
    forward(1, 2)
    x_relay(y)
    kv_forward(2)
    turn(y, 2)
    forward(0, 3)
    x_arrive(y, 3)
    turn(y, 3)
    for j in range(2):
        w_arrive((j, y, pc, z))
    pred[0, 0] = product(0, y, 0)
    pred[0, 1] = product(0, y, 2)
    forward(1, 3)
    pred[1, 0] = product(1, y, 0)
    pred[1, 1] = product(1, y, 2)
    x_relay(yo)

    def p_send(j):
        for r in range(4):
            for part in range(2):
                w_arrive((j, yo, part, zs[r]))
        if j == 0:
            x_arrive(yo, 3)
        p_out[j] = (pred[j, 1] + product(j, yo, 2)).astype(BF16).reshape(2, rows, chunk)
        for slot in range(2):
            push(p_out.at[j, slot], p_in.at[j, slot], sem_p.at[j, slot], xn_dev)

    p_send(0)
    p_send(1)
    pred[0, 0] += product(0, yo, 0)
    pred[1, 0] += product(1, yo, 0)

    ends = []
    total = 0
    for i in range(len_ref.shape[1]):
        total = total + len_ref[0, i]
        ends.append(total)

    def document(position):
        found = jnp.zeros(position.shape, jnp.int32)
        for end in ends:
            found = found + (position >= end).astype(jnp.int32)
        return found

    lanes = lax.broadcasted_iota(jnp.int32, (1, BLK), 1)
    k_pos = jnp.concatenate([asg_ref[0, j] * BLK + lanes for j in range(4)], axis=1)
    q_pos = asg_ref[0, z] * BLK + lax.broadcasted_iota(jnp.int32, (rows, 1), 0)
    allowed = (document(q_pos) == document(k_pos)) & (q_pos >= k_pos)
    kv_forward(3)
    k_all = kv_all[0].reshape(4 * rows, HD)
    v_all = kv_all[1].reshape(4 * rows, HD)

    def attend(h):
        scores = lax.dot_general(
            q_ref[:, h * HD : (h + 1) * HD], k_all, (((1,), (1,)), ((), ())),
            preferred_element_type=F32,
        ) * HD ** (-0.5)
        masked = jnp.where(allowed, scores, NEGATIVE)
        top = jnp.max(masked, axis=1, keepdims=True)
        terms = jnp.where(allowed, jnp.exp(masked - top), 0.0)
        totals = jnp.sum(terms, axis=1, keepdims=True)
        mixture = jnp.dot(terms.astype(BF16), v_all, preferred_element_type=F32)
        done = (mixture / totals).astype(BF16)
        att_ref[:, h * HD : (h + 1) * HD] = done
        att_half[h // 2, h % 2] = done

    def scale_rows(j, slot, attended):
        arrive(p_in.at[j, slot], sem_p.at[j, slot])
        factor = inv[slot]
        raw = pred[j, 0, slot * rows : (slot + 1) * rows, :] + p_in[j, slot].astype(F32)
        gap = raw * factor - attended.astype(F32)
        s_all[j, slot] = (gap * token_total ** (-0.5) * factor).astype(BF16)
        push(s_all.at[j, slot], s_all.at[j, slot + 2], sem_s.at[j, slot], xn_dev)

    for j in range(2):
        attend(j)
        attend(2 + j)
        push(att_half.at[pc, j], att_peer.at[j], sem_att.at[j], mate)
        scale_rows(j, 0, att_half[c, j])
        arrive(att_peer.at[j], sem_att.at[j])
        if j == 0:
            arrive(inv.at[1], sem_inv.at[0])
        scale_rows(j, 1, att_peer[j])
    turn(yo, 2)
    turn(yo, 3)

    def grad(j, at_y, first):
        return jnp.dot(
            xt[at_y, :, first * rows : (first + 2) * rows],
            s_all[j, first : first + 2].reshape(2 * rows, chunk),
            preferred_element_type=F32,
        ).reshape(2, 4, piece, chunk)

    order = (3, 2, 1, 0)
    for j in range(2):
        grad_f[j, 1] = grad(j, yo, 0)
        if j == 0:
            grad_f[0, 0] = grad(0, y, 0)
            grad_f[1, 0] = grad(1, y, 0)
        for slot in range(2):
            arrive(s_all.at[j, slot + 2], sem_s.at[j, slot])
        s_y[j] = (grad_f[j, 1] + grad(j, yo, 2)).astype(BF16)
        for r in order:
            for part in range(2):
                at = (j, part, zs[r])
                push(s_y.at[at], r_y.at[at], sem_ry.at[at], yn_dev)
        grad_f[j, 0] += grad(j, y, 2)

    def column_sum(j, part, g):
        at = (j, part, g)
        arrive(r_y.at[at], sem_ry.at[at])
        return grad_f[j, 0, part, g] + r_y[at].astype(F32)

    def z_push(j, part, g, dev):
        push(s_z.at[j, part, g], r_z.at[j, z, c], sem_rz.at[j, z, c], dev)

    for j in range(2):
        for r in order[:3]:
            g = zs[r]
            for part in range(2):
                s_z[j, part, g] = column_sum(j, part, g).astype(BF16)
            z_push(j, c, g, z_dev[r])
            z_push(j, pc, g, z_mate[r])
        for part in range(2):
            grad_f[j, 0, part, z] = column_sum(j, part, z)
        s_z[j, pc, z] = grad_f[j, 0, pc, z].astype(BF16)
        z_push(j, pc, z, mate)
    for j in range(2):
        total = grad_f[j, 0, c, z]
        for r in range(1, 4):
            arrive(r_z.at[j, zs[r], c], sem_rz.at[j, zs[r], c])
            total = total + r_z[j, zs[r], c].astype(F32)
        out_ref[:, cols(c, j)] = total
        total = jnp.zeros((piece, chunk), F32)
        for r in (3, 2, 1, 0):
            arrive(r_z.at[j, zs[r], pc], sem_rz.at[j, zs[r], pc])
            total = total + r_z[j, zs[r], pc].astype(F32)
        out_ref[:, cols(pc, j)] = total
    for copy in sent:
        copy.wait_send()
    for present, copy in sent_when:
        pl.when(present)(copy.wait_send)


def local_fused(student_in, weight, queries, keys, values, lengths, assignment):
    rows, width = student_in.shape
    piece, features = weight.shape
    chunk = features // 4
    depth = width // 4
    token_total = rows * lax.axis_size("dp") * lax.axis_size("seq")
    vmem = pl.BlockSpec(memory_space=pltpu.VMEM)
    smem = pl.BlockSpec(memory_space=pltpu.SMEM)
    dma = pltpu.SemaphoreType.DMA
    quarter = (2, 4, piece, chunk)
    return pl.pallas_call(
        functools.partial(fused_kernel, token_total),
        out_shape=(
            jax.ShapeDtypeStruct((rows, features), BF16),
            jax.ShapeDtypeStruct((piece, features), F32),
        ),
        in_specs=[vmem] * 5 + [smem] * 2,
        out_specs=(vmem, vmem),
        scratch_shapes=[
            pltpu.VMEM((2, 4, rows, depth), BF16),
            pltpu.VMEM((2, depth, 4 * rows), BF16),
            pltpu.VMEM((2, 2) + quarter, BF16),
            pltpu.VMEM((2, 4, rows, HD), BF16),
            pltpu.VMEM((2, rows, 128), F32),
            pltpu.VMEM((2, 2, 2 * rows, chunk), F32),
            pltpu.VMEM((2, 2, rows, chunk), BF16),
            pltpu.VMEM((2, 2, rows, chunk), BF16),
            pltpu.VMEM((2, 4, rows, chunk), BF16),
            pltpu.VMEM((2, 2, rows, chunk), BF16),
            pltpu.VMEM((2, rows, chunk), BF16),
            pltpu.VMEM((2, 2) + quarter, F32),
            pltpu.VMEM((2,) + quarter, BF16),
            pltpu.VMEM((2,) + quarter, BF16),
            pltpu.VMEM((2,) + quarter, BF16),
            pltpu.VMEM((2, 4, 2, piece, chunk), BF16),
            dma((96,)),
            dma((96,)),
            dma((2, 2, 2, 4)),
            dma((2, 4)),
            dma((2, 4)),
            dma((1,)),
            dma((2,)),
            dma((2, 2)),
            dma((2, 2)),
            dma((2, 2, 4)),
            dma((2, 4, 2)),
        ],
        compiler_params=pltpu.CompilerParams(collective_id=0, has_side_effects=True),
        name="distill",
    )(student_in, weight, queries, keys, values, lengths, assignment)


def fits(student_in, weight, queries, keys, values, lengths, assignment):
    rows, width = student_in.shape
    piece, features = weight.shape
    return (
        lax.axis_size("dp") == 8
        and lax.axis_size("seq") == 4
        and rows == BLK
        and assignment.shape[1] == 4
        and piece % 16 == 0
        and width == 32 * piece
        and width % 512 == 0
        and features == HQ * HD
        and keys.shape[1] == HD
    )


def dispatch(*arrays):
    return local_fused(*arrays) if fits(*arrays) else local(*arrays)


def solution(mesh):
    placed = (
        P(("dp", "seq"), None),
        P(("dp", "seq"), None),
        P(("dp", "seq"), None),
        P(("dp", "seq"), None),
        P(("dp", "seq"), None),
        P("dp", None),
        P("dp", None),
    )
    return jax.shard_map(
        dispatch,
        mesh=mesh,
        in_specs=placed,
        out_specs=(P(("dp", "seq"), None), P(("dp", "seq"), None)),
        check_vma=False,
    )
```

```python
import functools
import math

import jax
import jax.numpy as jnp
from jax import lax
from jax.experimental import pallas as pl
from jax.experimental.pallas import tpu as pltpu
from jax.sharding import PartitionSpec as P

HD = 128
HQ = 4
BLK = 128


EPSILON = 1e-06
NEGATIVE = -1e30


def locate(assign_row, doc_ends, first_slot, count):
    slot_ids = first_slot + jnp.arange(count, dtype=jnp.int32)
    block_ids = slot_ids // BLK
    block_table = jnp.arange(assign_row.shape[0], dtype=jnp.int32)
    placed = jnp.sum(
        jnp.where(block_ids[:, None] == block_table[None, :], assign_row[None, :], 0), axis=1
    )
    position = placed * BLK + slot_ids % BLK
    document = jnp.sum((position[:, None] >= doc_ends[None, :]).astype(jnp.int32), axis=1)
    return (position, document)


def absorb_block(state, key_block, value_block, query_heads, allowed):
    run_max, run_total, run_acc = state
    scores = jnp.einsum(
        "qhd,kd->hqk", query_heads, key_block, preferred_element_type=jnp.float32
    ) * HD ** (-0.5)
    masked = jnp.where(allowed[None], scores, NEGATIVE)
    new_max = jnp.maximum(run_max, jnp.max(masked, axis=-1))
    fading = jnp.exp(run_max - new_max)
    exp_terms = jnp.where(allowed[None], jnp.exp(masked - new_max[:, :, None]), 0.0)
    new_total = run_total * fading + jnp.sum(exp_terms, axis=-1)
    mixture = jnp.einsum(
        "hqk,kd->qhd",
        exp_terms.astype(jnp.bfloat16),
        value_block,
        preferred_element_type=jnp.float32,
    )
    new_acc = run_acc * fading.T[:, :, None] + mixture
    return (new_max, new_total, new_acc)


def local(student_in, weight, queries, keys, values, lengths, assignment):
    rows = queries.shape[0]
    assign_row = assignment[0]
    doc_ends = jnp.cumsum(lengths[0])
    query_pos, query_doc = locate(assign_row, doc_ends, lax.axis_index("seq") * rows, rows)
    query_heads = queries.reshape(rows, HQ, HD)
    start_state = (
        jnp.full((HQ, rows), NEGATIVE, jnp.float32),
        jnp.zeros((HQ, rows), jnp.float32),
        jnp.zeros((rows, HQ, HD), jnp.float32),
    )
    key_piece = lax.all_gather(keys, "seq", axis=0, tiled=True)
    value_piece = lax.all_gather(values, "seq", axis=0, tiled=True)
    count = key_piece.shape[0]
    step_rows = math.gcd(count, 512)
    steps_count = count // step_rows
    key_pos, key_doc = locate(assign_row, doc_ends, jnp.int32(0), count)

    def one_step(running, slabs):
        key_block, value_block, key_position, key_document = slabs
        allowed = (query_doc[:, None] == key_document[None, :]) & (
            query_pos[:, None] >= key_position[None, :]
        )
        updated = absorb_block(running, key_block, value_block, query_heads, allowed)
        return (updated, None)

    slabs = (
        key_piece.reshape(steps_count, step_rows, HD),
        value_piece.reshape(steps_count, step_rows, HD),
        key_pos.reshape(steps_count, step_rows),
        key_doc.reshape(steps_count, step_rows),
    )
    result, _ = lax.scan(one_step, start_state, slabs)
    final_max, final_total, final_acc = result
    attention = (final_acc / final_total.T[:, :, None]).reshape(rows, HQ * HD).astype(jnp.bfloat16)
    as_float = student_in.astype(jnp.float32)
    normed = (
        as_float * lax.rsqrt(jnp.mean(as_float * as_float, axis=1, keepdims=True) + EPSILON)
    ).astype(jnp.bfloat16)
    group_rows = lax.all_gather(weight, "seq", axis=0, tiled=True)
    columns = normed
    predicted = jnp.dot(
        columns,
        lax.all_gather(group_rows, "dp", axis=0, tiled=True),
        preferred_element_type=jnp.float32,
    )
    dp_count = lax.axis_size("dp")
    seq_count = lax.axis_size("seq")
    token_total = rows * dp_count * seq_count
    scaled = ((predicted - attention.astype(jnp.float32)) * token_total ** (-0.5)).astype(
        jnp.bfloat16
    )
    columns = normed
    outer_rows = lax.psum_scatter(
        lax.dot_general(
            columns, scaled, (((0,), (0,)), ((), ())), preferred_element_type=jnp.float32
        ).astype(jnp.bfloat16),
        "dp",
        scatter_dimension=0,
        tiled=True,
    )
    weight_grad = lax.psum_scatter(outer_rows, "seq", scatter_dimension=0, tiled=True).astype(
        jnp.float32
    )
    return (attention, weight_grad)


MESH = pl.DeviceIdType.MESH
F32 = jnp.float32
BF16 = jnp.bfloat16


def fused_kernel(
    token_total,
    x_hbm, w_hbm, q_hbm, k_hbm, v_hbm, len_hbm, asg_hbm,
    att_ref, out_ref,
    xs, xo, xt, w_all, w_peer, q_ref, kv_all, len_ref, asg_ref, inv, inv_row, pred, p_out, p_in,
    s_all, att_half, att_peer, grad_f, s_y, r_y, s_z, r_z, bulk,
    local_sem, send, sem_w, sem_w_far, sem_kv, sem_x, sem_inv, sem_att, sem_p, sem_ry, sem_rz,
):
    rows = q_ref.shape[0]
    piece = w_hbm.shape[0]
    half = w_hbm.shape[1] // 2
    chunk = half // 2
    depth = xs.shape[3]
    dp, z = lax.axis_index("dp"), lax.axis_index("seq")
    c = dp % 2
    pc = 1 - c
    x = (dp // 2) % 2
    y = dp // 4
    yo = 1 - y
    dp_m = dp + 1 - 2 * c
    mate = (dp_m, z)
    xn_dev = (dp + 2 - 4 * x, z)
    xn_mate = (dp_m + 2 - 4 * x, z)
    yn_dev = (dp + 4 - 8 * y, z)
    yn_mate = (dp_m + 4 - 8 * y, z)
    zs = (z, z + 1 - 2 * (z % 2), z + 2 - 4 * (z // 2), 3 - z)
    mid = ((z + 1) // 2) % 2
    z_two = mid * zs[3] + (1 - mid) * zs[2]
    z_from = (
        mid * zs[3] + (1 - mid) * zs[1],
        mid * zs[1] + (1 - mid) * zs[2],
        mid * zs[2] + (1 - mid) * zs[3],
    )
    z_dev = [(dp, zs[r]) for r in range(4)]
    z_mate = [(dp_m, zs[r]) for r in range(4)]

    def cols(core, j):
        return pl.ds(pl.multiple_of(core * half + j * chunk, 128), chunk)

    def width(at_y, at_x):
        return pl.ds(pl.multiple_of((at_y * 2 + at_x) * depth, 128), depth)

    barrier = pltpu.get_barrier_semaphore()
    greeted = [mate, xn_dev, xn_mate, yn_dev, yn_mate] + z_dev[1:] + z_mate[1:]
    for dev in greeted:
        pl.semaphore_signal(barrier, inc=1, device_id=dev, device_id_type=MESH)

    def lines(ref):
        return math.prod(ref.shape) * jnp.dtype(ref.dtype).itemsize // 256

    def fetch(at, *pairs):
        copies = [pltpu.make_async_copy(a, b, local_sem.at[at]) for a, b in pairs]
        for copy in copies:
            copy.start()
        return sum(lines(b) for _, b in pairs)

    def amount(count, sem):
        part = bulk.at[pl.ds(0, count)]
        return pltpu.make_async_copy(part, part, sem)

    get_w = [
        fetch(
            j,
            (w_hbm.at[:, cols(c, j)], w_all.at[j, y, c, z]),
            (w_hbm.at[:, cols(pc, j)], w_peer.at[j]),
        )
        for j in range(2)
    ]
    get_xo = [
        fetch(2 + i, (x_hbm.at[:, width(at, 1 - x)], xo.at[at])) for i, at in enumerate((y, yo))
    ]
    get_kv = fetch(4, *((ref, kv_all.at[i, z]) for i, ref in enumerate((k_hbm, v_hbm))))
    get_xs = fetch(5, *((x_hbm.at[:, width(at, x)], xs.at[at, 0]) for at in (y, yo)))
    fetch(6, (q_hbm, q_ref))
    fetch(7, (len_hbm, len_ref))
    fetch(8, (asg_hbm, asg_ref))
    pl.semaphore_wait(barrier, len(greeted))

    sent = [0, 0, 0, 0, 0]

    def push(src, dst, rsem, dev, group, counted=True):
        copy = pltpu.make_async_remote_copy(
            src_ref=src, dst_ref=dst, send_sem=send.at[group], recv_sem=rsem,
            device_id=dev, device_id_type=MESH,
        )
        copy.start()
        if counted:
            sent[group] += lines(src)

    def arrive(dst, rsem):
        pltpu.make_async_remote_copy(
            src_ref=dst, dst_ref=dst, send_sem=send.at[0], recv_sem=rsem,
            device_id=mate, device_id_type=MESH,
        ).wait_recv()

    def w_start(j):
        at = (j, y, c, z)
        dst, sem = w_all.at[at], sem_w.at[j, c, z]
        amount(get_w[j], local_sem.at[j]).wait()
        push(dst, dst, sem, (dp, z_two), 0)
        push(w_peer.at[j], dst, sem, (dp_m, z_two), 0)
        push(dst, dst, sem, z_dev[1], 0)
        push(w_peer.at[j], dst, sem, z_mate[1], 0)
        push(dst, dst, sem_w_far.at[j], yn_dev, 0)
        push(w_peer.at[j], dst, sem_w_far.at[j], yn_mate, 0)
        push(w_peer.at[j], dst, sem, mate, 0)

    w_start(0)
    for i, at_y in enumerate((y, yo)):
        amount(get_xo[i], local_sem.at[2 + i]).wait()
        push(xo.at[at_y], xs.at[at_y, 2], sem_x.at[at_y, 2], xn_dev, 1)
    amount(get_kv, local_sem.at[4]).wait()
    kv_own = kv_all.at[:, z]
    push(kv_own, kv_own, sem_kv.at[z], (dp, z_two), 2)
    push(kv_own, kv_own, sem_kv.at[z], z_dev[1], 2)
    w_start(1)
    amount(get_xs, local_sem.at[5]).wait()
    push(xs.at[:, 0], xs.at[:, 1], sem_x.at[0, 1], mate, 1)

    step = 16

    @pl.loop(0, rows // step)
    def _(i):
        at = pl.ds(pl.multiple_of(i * step, step), step)
        total = jnp.zeros((step, 1), F32)
        for ref in (xs.at[0, 0], xs.at[1, 0], xo.at[0], xo.at[1]):
            block = ref[at, :].astype(F32)
            total = total + jnp.sum(block * block, axis=1, keepdims=True)
        factor = lax.rsqrt(total / (4 * depth) + EPSILON)
        inv[0, at, :] = jnp.broadcast_to(factor, (step, 128))

    inv_row[0] = inv[0].T[:8]
    push(inv_row.at[0], inv_row.at[1], sem_inv.at[0], mate, 2)
    push(inv_row.at[0], inv_row.at[2], sem_inv.at[1], xn_dev, 2)
    push(inv_row.at[0], inv_row.at[3], sem_inv.at[1], xn_mate, 2)

    relayed = []

    def relay(ref, sem, k, where):
        if k == 1 or where == 0:
            return
        copy = pltpu.make_async_remote_copy(
            src_ref=ref, dst_ref=ref, send_sem=send.at[5], recv_sem=sem,
            device_id=z_dev[1], device_id_type=MESH,
        )
        if where == 1:
            copy.start()
        else:
            pl.when(mid == 1)(copy.start)
        relayed.append(lines(ref))

    def forward(j, k, where=None):
        for part in range(2):
            at = (j, y, part, z_from[k])
            arrive(w_all.at[at], sem_w.at[j, part, z_from[k]])
            relay(w_all.at[at], sem_w.at[j, part, z_from[k]], k, where)
            push(w_all.at[at], w_all.at[at], sem_w_far.at[j], yn_dev, 3, where != 1)

    def kv_forward(k, where):
        at = kv_all.at[:, z_from[k]]
        arrive(at, sem_kv.at[z_from[k]])
        relay(at, sem_kv.at[z_from[k]], k, where)

    def x_arrive(at_y, slot):
        arrive(xs.at[at_y, slot], sem_x.at[at_y, slot])

    def x_relay(at_y):
        x_arrive(at_y, 2)
        push(xs.at[at_y, 2], xs.at[at_y, 3], sem_x.at[at_y, 3], mate, 2)

    def turn(at_y, slot):
        for j in range(depth // 128):
            at = slice(j * 128, (j + 1) * 128)
            xt[at_y, at, slot * rows : (slot + 1) * rows] = xs[at_y, slot, :, at].T

    def product(j, at_y, first):
        return jnp.dot(
            xs[at_y, first : first + 2].reshape(2 * rows, depth),
            w_all[j, at_y].reshape(depth, chunk),
            preferred_element_type=F32,
        )

    arrive(xs.at[:, 1], sem_x.at[0, 1])
    for slot in range(2):

        @pl.loop(0, 2)
        def _(at_y):
            turn(at_y, slot)

    def spread(slot):
        inv[slot] = jnp.broadcast_to(inv_row[slot, :1], (rows, 128)).T

    for k in range(3):
        forward(0, k)

    @pl.when(mid == 1)
    def _():
        for k in range(3):
            kv_forward(k, 1)

    x_relay(y)
    arrive(inv_row.at[1], sem_inv.at[0])
    spread(1)
    for j in range(2):
        arrive(w_all.at[j, y, pc, z], sem_w.at[j, pc, z])
    pred[0, 0] = product(0, y, 0)
    turn(y, 2)
    x_arrive(y, 3)
    turn(y, 3)
    pred[0, 1] = product(0, y, 2)
    for at in (6, 7, 8):
        ref = (q_ref, len_ref, asg_ref)[at - 6]
        pltpu.make_async_copy((q_hbm, len_hbm, asg_hbm)[at - 6], ref, local_sem.at[at]).wait()

    @pl.when(mid == 1)
    def _():
        for k in range(3):
            forward(1, k, 1)

    @pl.when(mid == 0)
    def _():
        forward(1, 0, 0)
        for k in range(3):
            kv_forward(k, 0)

    ends = []
    total = 0
    for i in range(len_ref.shape[1]):
        total = total + len_ref[0, i]
        ends.append(total)

    def document(position):
        found = jnp.zeros(position.shape, jnp.int32)
        for end in ends:
            found = found + (position >= end).astype(jnp.int32)
        return found

    lanes = lax.broadcasted_iota(jnp.int32, (1, BLK), 1)
    k_pos = jnp.concatenate([asg_ref[0, j] * BLK + lanes for j in range(4)], axis=1)
    q_pos = asg_ref[0, z] * BLK + lax.broadcasted_iota(jnp.int32, (rows, 1), 0)
    allowed = (document(q_pos) == document(k_pos)) & (q_pos >= k_pos)

    def attend(h):
        k_all = kv_all[0].reshape(4 * rows, HD)
        v_all = kv_all[1].reshape(4 * rows, HD)
        scores = lax.dot_general(
            q_ref[:, h * HD : (h + 1) * HD], k_all, (((1,), (1,)), ((), ())),
            preferred_element_type=F32,
        ) * HD ** (-0.5)
        masked = jnp.where(allowed, scores, NEGATIVE)
        top = jnp.max(masked, axis=1, keepdims=True)
        terms = jnp.where(allowed, jnp.exp(masked - top), 0.0)
        totals = jnp.sum(terms, axis=1, keepdims=True)
        mixture = jnp.dot(terms.astype(BF16), v_all, preferred_element_type=F32)
        done = (mixture / totals).astype(BF16)
        att_ref[:, h * HD : (h + 1) * HD] = done
        att_half[h // 2, h % 2] = done

    def part_send(j, slot, value):
        p_out[j, slot] = value.astype(BF16)
        at = (j, (slot + 2) % 4)
        push(p_out.at[j, slot], p_in.at[at], sem_p.at[at], xn_dev, 2)

    def fold(j, slot, attended):
        at = slice(slot * rows, (slot + 1) * rows)
        value = pred[j, 0, at, :] - attended.astype(F32) / inv[slot]
        pred[j, 0, at, :] = value
        part_send(j, slot, value)

    def exchange(j):
        arrive(w_all.at[j, yo], sem_w_far.at[j])
        pred[j, 0] += product(j, yo, 0)
        fold(j, 0, att_half[c, j])
        arrive(att_peer.at[j], sem_att.at[j])
        fold(j, 1, att_peer[j])
        if j == 0:
            x_arrive(yo, 3)
        pred[j, 1] += product(j, yo, 2)
        for slot in range(2):
            part_send(j, 2 + slot, pred[j, 1, slot * rows : (slot + 1) * rows, :])

    attend(0)
    x_relay(yo)
    attend(2)
    push(att_half.at[pc, 0], att_peer.at[0], sem_att.at[0], mate, 2)
    exchange(0)

    @pl.when(mid == 0)
    def _():
        forward(1, 1, 0)
        forward(1, 2, 0)

    attend(1)
    attend(3)
    push(att_half.at[pc, 1], att_peer.at[1], sem_att.at[1], mate, 2)
    pred[1, 0] = product(1, y, 0)
    pred[1, 1] = product(1, y, 2)
    turn(yo, 2)
    turn(yo, 3)
    arrive(inv_row.at[2:4], sem_inv.at[1])
    spread(2)
    spread(3)
    exchange(1)

    def scale_rows(j, slot):
        arrive(p_in.at[j, slot], sem_p.at[j, slot])
        at = slice((slot % 2) * rows, (slot % 2 + 1) * rows)
        factor = inv[slot]
        raw = pred[j, slot // 2, at, :] + p_in[j, slot].astype(F32)
        s_all[j, slot] = (raw * factor * (factor * token_total ** (-0.5))).astype(BF16)

    def grad(j, at_y):
        return jnp.dot(
            xt[at_y], s_all[j].reshape(4 * rows, chunk), preferred_element_type=F32
        ).reshape(2, 4, piece, chunk)

    order = (3, 2, 1, 0)
    for j in range(2):
        for slot in (2, 3, 0, 1):
            scale_rows(j, slot)
        s_y[j] = grad(j, yo).astype(BF16)
        for r in order:
            at = (j, slice(None), zs[r])
            push(s_y.at[at], r_y.at[at], sem_ry.at[j, zs[r]], yn_dev, 4)
        grad_f[j] = grad(j, y)

    def column_sum(j, part, g):
        return grad_f[j, part, g] + r_y[j, part, g].astype(F32)

    def z_push(j, part, g, dev):
        push(s_z.at[j, part, g], r_z.at[j, z, c], sem_rz.at[j], dev, 4)

    for j in range(2):
        for r in order[:3]:
            g = zs[r]
            arrive(r_y.at[j, :, g], sem_ry.at[j, g])
            for part in range(2):
                s_z[j, part, g] = column_sum(j, part, g).astype(BF16)
            z_push(j, c, g, z_dev[r])
            z_push(j, pc, g, z_mate[r])
        arrive(r_y.at[j, :, z], sem_ry.at[j, z])
        for part in range(2):
            grad_f[j, part, z] = column_sum(j, part, z)
        s_z[j, pc, z] = grad_f[j, pc, z].astype(BF16)
        z_push(j, pc, z, mate)
    for j in range(2):
        amount(7 * piece, sem_rz.at[j]).wait()
        total = grad_f[j, c, z]
        for r in range(1, 4):
            total = total + r_z[j, zs[r], c].astype(F32)
        out_ref[:, cols(c, j)] = total
        total = jnp.zeros((piece, chunk), F32)
        for r in (3, 2, 1, 0):
            total = total + r_z[j, zs[r], pc].astype(F32)
        out_ref[:, cols(pc, j)] = total
    for group in range(5):
        amount(sent[group], send.at[group]).wait()
    pl.when(mid == 1)(amount(sum(relayed), send.at[5]).wait)


def local_fused(student_in, weight, queries, keys, values, lengths, assignment):
    rows, width = student_in.shape
    piece, features = weight.shape
    chunk = features // 4
    depth = width // 4
    token_total = rows * lax.axis_size("dp") * lax.axis_size("seq")
    vmem = pl.BlockSpec(memory_space=pltpu.VMEM)
    hbm = pl.BlockSpec(memory_space=pltpu.HBM)
    dma = pltpu.SemaphoreType.DMA
    quarter = (2, 4, piece, chunk)
    return pl.pallas_call(
        functools.partial(fused_kernel, token_total),
        out_shape=(
            pltpu.VMEM((rows, features), BF16),
            pltpu.VMEM((piece, features), F32),
        ),
        in_specs=[hbm] * 7,
        out_specs=(vmem, vmem),
        scratch_shapes=[
            pltpu.VMEM((2, 4, rows, depth), BF16),
            pltpu.VMEM((2, rows, depth), BF16),
            pltpu.VMEM((2, depth, 4 * rows), BF16),
            pltpu.VMEM((2, 2) + quarter, BF16),
            pltpu.VMEM((2, piece, chunk), BF16),
            pltpu.VMEM((rows, features), BF16),
            pltpu.VMEM((2, 4, rows, HD), BF16),
            pltpu.SMEM(lengths.shape, jnp.int32),
            pltpu.SMEM(assignment.shape, jnp.int32),
            pltpu.VMEM((4, rows, 128), F32),
            pltpu.VMEM((4, 8, 128), F32),
            pltpu.VMEM((2, 2, 2 * rows, chunk), F32),
            pltpu.VMEM((2, 4, rows, chunk), BF16),
            pltpu.VMEM((2, 4, rows, chunk), BF16),
            pltpu.VMEM((2, 4, rows, chunk), BF16),
            pltpu.VMEM((2, 2, rows, chunk), BF16),
            pltpu.VMEM((2, rows, chunk), BF16),
            pltpu.VMEM((2,) + quarter, F32),
            pltpu.VMEM((2,) + quarter, BF16),
            pltpu.VMEM((2,) + quarter, BF16),
            pltpu.VMEM((2,) + quarter, BF16),
            pltpu.VMEM((2, 4, 2, piece, chunk), BF16),
            pltpu.VMEM((8192, 128), BF16),
            dma((9,)),
            dma((6,)),
            dma((2, 2, 4)),
            dma((2,)),
            dma((4,)),
            dma((2, 4)),
            dma((2,)),
            dma((2,)),
            dma((2, 4)),
            dma((2, 4)),
            dma((2,)),
        ],
        compiler_params=pltpu.CompilerParams(collective_id=0, has_side_effects=True),
        name="distill",
    )(student_in, weight, queries, keys, values, lengths, assignment)


def fits(student_in, weight, queries, keys, values, lengths, assignment):
    rows, width = student_in.shape
    piece, features = weight.shape
    return (
        lax.axis_size("dp") == 8
        and lax.axis_size("seq") == 4
        and rows == BLK
        and assignment.shape[1] == 4
        and piece % 16 == 0
        and width == 32 * piece
        and width % 512 == 0
        and features == HQ * HD
        and keys.shape[1] == HD
    )


def dispatch(*arrays):
    return local_fused(*arrays) if fits(*arrays) else local(*arrays)


def solution(mesh):
    placed = (
        P(("dp", "seq"), None),
        P(("dp", "seq"), None),
        P(("dp", "seq"), None),
        P(("dp", "seq"), None),
        P(("dp", "seq"), None),
        P("dp", None),
        P("dp", None),
    )
    return jax.shard_map(
        dispatch,
        mesh=mesh,
        in_specs=placed,
        out_specs=(P(("dp", "seq"), None), P(("dp", "seq"), None)),
        check_vma=False,
    )
```

```python
import functools
import math

import jax
import jax.numpy as jnp
from jax import lax
from jax.experimental import pallas as pl
from jax.experimental.pallas import tpu as pltpu
from jax.sharding import PartitionSpec as P

HD = 128
HQ = 4
BLK = 128


EPSILON = 1e-06
NEGATIVE = -1e30


def locate(assign_row, doc_ends, first_slot, count):
    slot_ids = first_slot + jnp.arange(count, dtype=jnp.int32)
    block_ids = slot_ids // BLK
    block_table = jnp.arange(assign_row.shape[0], dtype=jnp.int32)
    placed = jnp.sum(
        jnp.where(block_ids[:, None] == block_table[None, :], assign_row[None, :], 0), axis=1
    )
    position = placed * BLK + slot_ids % BLK
    document = jnp.sum((position[:, None] >= doc_ends[None, :]).astype(jnp.int32), axis=1)
    return (position, document)


def absorb_block(state, key_block, value_block, query_heads, allowed):
    run_max, run_total, run_acc = state
    scores = jnp.einsum(
        "qhd,kd->hqk", query_heads, key_block, preferred_element_type=jnp.float32
    ) * HD ** (-0.5)
    masked = jnp.where(allowed[None], scores, NEGATIVE)
    new_max = jnp.maximum(run_max, jnp.max(masked, axis=-1))
    fading = jnp.exp(run_max - new_max)
    exp_terms = jnp.where(allowed[None], jnp.exp(masked - new_max[:, :, None]), 0.0)
    new_total = run_total * fading + jnp.sum(exp_terms, axis=-1)
    mixture = jnp.einsum(
        "hqk,kd->qhd",
        exp_terms.astype(jnp.bfloat16),
        value_block,
        preferred_element_type=jnp.float32,
    )
    new_acc = run_acc * fading.T[:, :, None] + mixture
    return (new_max, new_total, new_acc)


def local(student_in, weight, queries, keys, values, lengths, assignment):
    rows = queries.shape[0]
    assign_row = assignment[0]
    doc_ends = jnp.cumsum(lengths[0])
    query_pos, query_doc = locate(assign_row, doc_ends, lax.axis_index("seq") * rows, rows)
    query_heads = queries.reshape(rows, HQ, HD)
    start_state = (
        jnp.full((HQ, rows), NEGATIVE, jnp.float32),
        jnp.zeros((HQ, rows), jnp.float32),
        jnp.zeros((rows, HQ, HD), jnp.float32),
    )
    key_piece = lax.all_gather(keys, "seq", axis=0, tiled=True)
    value_piece = lax.all_gather(values, "seq", axis=0, tiled=True)
    count = key_piece.shape[0]
    step_rows = math.gcd(count, 512)
    steps_count = count // step_rows
    key_pos, key_doc = locate(assign_row, doc_ends, jnp.int32(0), count)

    def one_step(running, slabs):
        key_block, value_block, key_position, key_document = slabs
        allowed = (query_doc[:, None] == key_document[None, :]) & (
            query_pos[:, None] >= key_position[None, :]
        )
        updated = absorb_block(running, key_block, value_block, query_heads, allowed)
        return (updated, None)

    slabs = (
        key_piece.reshape(steps_count, step_rows, HD),
        value_piece.reshape(steps_count, step_rows, HD),
        key_pos.reshape(steps_count, step_rows),
        key_doc.reshape(steps_count, step_rows),
    )
    result, _ = lax.scan(one_step, start_state, slabs)
    final_max, final_total, final_acc = result
    attention = (final_acc / final_total.T[:, :, None]).reshape(rows, HQ * HD).astype(jnp.bfloat16)
    as_float = student_in.astype(jnp.float32)
    normed = (
        as_float * lax.rsqrt(jnp.mean(as_float * as_float, axis=1, keepdims=True) + EPSILON)
    ).astype(jnp.bfloat16)
    group_rows = lax.all_gather(weight, "seq", axis=0, tiled=True)
    columns = normed
    predicted = jnp.dot(
        columns,
        lax.all_gather(group_rows, "dp", axis=0, tiled=True),
        preferred_element_type=jnp.float32,
    )
    dp_count = lax.axis_size("dp")
    seq_count = lax.axis_size("seq")
    token_total = rows * dp_count * seq_count
    scaled = ((predicted - attention.astype(jnp.float32)) * token_total ** (-0.5)).astype(
        jnp.bfloat16
    )
    columns = normed
    outer_rows = lax.psum_scatter(
        lax.dot_general(
            columns, scaled, (((0,), (0,)), ((), ())), preferred_element_type=jnp.float32
        ).astype(jnp.bfloat16),
        "dp",
        scatter_dimension=0,
        tiled=True,
    )
    weight_grad = lax.psum_scatter(outer_rows, "seq", scatter_dimension=0, tiled=True).astype(
        jnp.float32
    )
    return (attention, weight_grad)


MESH = pl.DeviceIdType.MESH
F32 = jnp.float32
BF16 = jnp.bfloat16


def fused_kernel(
    token_total,
    x_hbm, w_hbm, q_hbm, k_hbm, v_hbm, len_hbm, asg_hbm,
    att_ref, out_ref,
    xs, xo, xt, w_all, w_peer, q_ref, kv_all, len_ref, asg_ref, inv, inv_row, pred, p_out, p_in,
    s_all, att_half, att_peer, grad_f, s_y, r_y, s_z, r_z, bulk,
    local_sem, send, sem_w, sem_w_far, sem_kv, sem_x, sem_inv, sem_att, sem_p, sem_ry, sem_rz,
):
    rows = q_ref.shape[0]
    piece = w_hbm.shape[0]
    half = w_hbm.shape[1] // 2
    chunk = half // 2
    depth = xs.shape[3]
    dp, z = lax.axis_index("dp"), lax.axis_index("seq")
    c = dp % 2
    pc = 1 - c
    x = (dp // 2) % 2
    y = dp // 4
    yo = 1 - y
    dp_m = dp + 1 - 2 * c
    mate = (dp_m, z)
    xn_dev = (dp + 2 - 4 * x, z)
    xn_mate = (dp_m + 2 - 4 * x, z)
    yn_dev = (dp + 4 - 8 * y, z)
    yn_mate = (dp_m + 4 - 8 * y, z)
    zs = (z, z + 1 - 2 * (z % 2), z + 2 - 4 * (z // 2), 3 - z)
    mid = ((z + 1) // 2) % 2
    z_two = mid * zs[3] + (1 - mid) * zs[2]
    z_from = (
        mid * zs[3] + (1 - mid) * zs[1],
        zs[2],
        mid * zs[1] + (1 - mid) * zs[3],
    )
    z_dev = [(dp, zs[r]) for r in range(4)]
    z_mate = [(dp_m, zs[r]) for r in range(4)]

    def cols(core, j):
        return pl.ds(pl.multiple_of(core * half + j * chunk, 128), chunk)

    def width(at_y, at_x):
        return pl.ds(pl.multiple_of((at_y * 2 + at_x) * depth, 128), depth)

    barrier = pltpu.get_barrier_semaphore()
    greeted = [mate, xn_dev, xn_mate, yn_dev, yn_mate] + z_dev[1:] + z_mate[1:]
    for dev in greeted:
        pl.semaphore_signal(barrier, inc=1, device_id=dev, device_id_type=MESH)

    def lines(ref):
        return math.prod(ref.shape) * jnp.dtype(ref.dtype).itemsize // 256

    def fetch(at, *pairs):
        copies = [pltpu.make_async_copy(a, b, local_sem.at[at]) for a, b in pairs]
        for copy in copies:
            copy.start()
        return sum(lines(b) for _, b in pairs)

    def amount(count, sem):
        part = bulk.at[pl.ds(0, count)]
        return pltpu.make_async_copy(part, part, sem)

    get_w = [
        fetch(
            j,
            (w_hbm.at[:, cols(c, j)], w_all.at[j, y, c, z]),
            (w_hbm.at[:, cols(pc, j)], w_peer.at[j]),
        )
        for j in range(2)
    ]
    get_xo = [
        fetch(2 + i, (x_hbm.at[:, width(at, 1 - x)], xo.at[at])) for i, at in enumerate((y, yo))
    ]
    get_kv = fetch(4, *((ref, kv_all.at[i, z]) for i, ref in enumerate((k_hbm, v_hbm))))
    get_xs = fetch(5, *((x_hbm.at[:, width(at, x)], xs.at[at, 0]) for at in (y, yo)))
    fetch(6, (q_hbm, q_ref))
    fetch(7, (len_hbm, len_ref))
    fetch(8, (asg_hbm, asg_ref))
    pl.semaphore_wait(barrier, len(greeted))

    sent = [0, 0, 0, 0, 0]

    def push(src, dst, rsem, dev, group, counted=True):
        copy = pltpu.make_async_remote_copy(
            src_ref=src, dst_ref=dst, send_sem=send.at[group], recv_sem=rsem,
            device_id=dev, device_id_type=MESH,
        )
        copy.start()
        if counted:
            sent[group] += lines(src)

    def arrive(dst, rsem):
        pltpu.make_async_remote_copy(
            src_ref=dst, dst_ref=dst, send_sem=send.at[0], recv_sem=rsem,
            device_id=mate, device_id_type=MESH,
        ).wait_recv()

    def w_along(j, to):
        dst, sem = w_all.at[j, y, c, z], sem_w.at[j, z]
        push(dst, dst, sem, (dp, to), 0)
        push(w_peer.at[j], dst, sem, (dp_m, to), 0)

    def w_across(j):
        dst, sem = w_all.at[j, y, c, z], sem_w.at[j, z]
        push(dst, dst, sem_w_far.at[j], yn_dev, 0)
        push(w_peer.at[j], dst, sem_w_far.at[j], yn_mate, 0)
        push(w_peer.at[j], dst, sem, mate, 0)

    kv_own = kv_all.at[:, z]
    amount(get_w[0], local_sem.at[0]).wait()
    w_along(0, z_two)
    w_along(0, zs[1])
    w_across(0)
    amount(get_kv, local_sem.at[4]).wait()
    push(kv_own, kv_own, sem_kv.at[z], (dp, z_two), 2)
    push(kv_own, kv_own, sem_kv.at[z], z_dev[1], 2)
    for i, at_y in enumerate((y, yo)):
        amount(get_xo[i], local_sem.at[2 + i]).wait()
        push(xo.at[at_y], xs.at[at_y, 2], sem_x.at[at_y, 0], xn_dev, 1)
    amount(get_w[1], local_sem.at[1]).wait()
    w_along(1, z_two)
    w_along(1, zs[1])
    w_across(1)
    amount(get_xs, local_sem.at[5]).wait()
    push(xs.at[:, 0], xs.at[:, 1], sem_x.at[0, 2], mate, 1)

    step = 16

    @pl.loop(0, rows // step)
    def _(i):
        at = pl.ds(pl.multiple_of(i * step, step), step)
        total = jnp.zeros((step, 1), F32)
        for ref in (xs.at[0, 0], xs.at[1, 0], xo.at[0], xo.at[1]):
            block = ref[at, :].astype(F32)
            total = total + jnp.sum(block * block, axis=1, keepdims=True)
        factor = lax.rsqrt(total / (4 * depth) + EPSILON)
        inv[0, at, :] = jnp.broadcast_to(factor, (step, 128))

    inv_row[0] = inv[0].T[:8]
    push(inv_row.at[0], inv_row.at[1], sem_inv.at[0], mate, 2)
    push(inv_row.at[0], inv_row.at[2], sem_inv.at[1], xn_dev, 2)
    push(inv_row.at[0], inv_row.at[3], sem_inv.at[1], xn_mate, 2)

    relayed = []

    def relay(ref, sem, k, where):
        if k == 2 or where == 0:
            return
        copy = pltpu.make_async_remote_copy(
            src_ref=ref, dst_ref=ref, send_sem=send.at[5], recv_sem=sem,
            device_id=z_dev[1], device_id_type=MESH,
        )
        if where == 1:
            copy.start()
        else:
            pl.when(mid == 1)(copy.start)
        relayed.append(lines(ref))

    def forward(j, k, where=None):
        at = w_all.at[j, y, :, z_from[k]]
        arrive(at, sem_w.at[j, z_from[k]])
        relay(at, sem_w.at[j, z_from[k]], k, where)
        push(at, at, sem_w_far.at[j], yn_dev, 3, where != 1)

    def kv_forward(k, where):
        at = kv_all.at[:, z_from[k]]
        arrive(at, sem_kv.at[z_from[k]])
        relay(at, sem_kv.at[z_from[k]], k, where)

    def x_arrive(at_y, slot):
        arrive(xs.at[at_y, slot], sem_x.at[at_y, slot - 2])

    def x_relay(at_y):
        x_arrive(at_y, 2)
        push(xs.at[at_y, 2], xs.at[at_y, 3], sem_x.at[at_y, 1], mate, 2)

    def turn(at_y, slot):
        for j in range(depth // 128):
            at = slice(j * 128, (j + 1) * 128)
            xt[at_y, at, slot * rows : (slot + 1) * rows] = xs[at_y, slot, :, at].T

    def product(j, at_y, first):
        return jnp.dot(
            xs[at_y, first : first + 2].reshape(2 * rows, depth),
            w_all[j, at_y].reshape(depth, chunk),
            preferred_element_type=F32,
        )

    arrive(xs.at[:, 1], sem_x.at[0, 2])
    for slot in range(2):

        @pl.loop(0, 2)
        def _(at_y):
            turn(at_y, slot)

    def spread(slot):
        inv[slot] = jnp.broadcast_to(inv_row[slot, :1], (rows, 128)).T

    for k in range(3):
        forward(0, k)
    for j in range(2):
        arrive(w_all.at[j, y, pc, z], sem_w.at[j, z])
    pred[0, 0] = product(0, y, 0)

    @pl.when(mid == 1)
    def _():
        for k in range(3):
            kv_forward(k, 1)

    x_relay(y)
    arrive(inv_row.at[1], sem_inv.at[0])
    spread(1)
    for at in (6, 7, 8):
        ref = (q_ref, len_ref, asg_ref)[at - 6]
        pltpu.make_async_copy((q_hbm, len_hbm, asg_hbm)[at - 6], ref, local_sem.at[at]).wait()

    def near_rows():
        turn(y, 2)
        x_arrive(y, 3)
        turn(y, 3)
        pred[0, 1] = product(0, y, 2)

    @pl.when(mid == 0)
    def _():
        near_rows()
        forward(1, 0, 0)
        for k in range(3):
            kv_forward(k, 0)

    ends = []
    total = 0
    for i in range(len_ref.shape[1]):
        total = total + len_ref[0, i]
        ends.append(total)

    def document(position):
        found = jnp.zeros(position.shape, jnp.int32)
        for end in ends:
            found = found + (position >= end).astype(jnp.int32)
        return found

    lanes = lax.broadcasted_iota(jnp.int32, (1, BLK), 1)
    k_pos = jnp.concatenate([asg_ref[0, j] * BLK + lanes for j in range(4)], axis=1)
    q_pos = asg_ref[0, z] * BLK + lax.broadcasted_iota(jnp.int32, (rows, 1), 0)
    allowed = (document(q_pos) == document(k_pos)) & (q_pos >= k_pos)

    def attend(h):
        k_all = kv_all[0].reshape(4 * rows, HD)
        v_all = kv_all[1].reshape(4 * rows, HD)
        scores = lax.dot_general(
            q_ref[:, h * HD : (h + 1) * HD], k_all, (((1,), (1,)), ((), ())),
            preferred_element_type=F32,
        ) * HD ** (-0.5)
        masked = jnp.where(allowed, scores, NEGATIVE)
        top = jnp.max(masked, axis=1, keepdims=True)
        terms = jnp.where(allowed, jnp.exp(masked - top), 0.0)
        totals = jnp.sum(terms, axis=1, keepdims=True)
        mixture = jnp.dot(terms.astype(BF16), v_all, preferred_element_type=F32)
        done = (mixture / totals).astype(BF16)
        att_ref[:, h * HD : (h + 1) * HD] = done
        att_half[h // 2, h % 2] = done

    def part_send(j, slot, value):
        p_out[j, slot] = value.astype(BF16)
        at = (j, (slot + 2) % 4)
        push(p_out.at[j, slot], p_in.at[at], sem_p.at[at], xn_dev, 2)

    def fold(j, slot, attended):
        at = slice(slot * rows, (slot + 1) * rows)
        value = pred[j, 0, at, :] - attended.astype(F32) / inv[slot]
        pred[j, 0, at, :] = value
        part_send(j, slot, value)

    def fold_first(j):
        arrive(w_all.at[j, yo], sem_w_far.at[j])
        pred[j, 0] += product(j, yo, 0)
        fold(j, 0, att_half[c, j])

    def fold_second(j):
        arrive(att_peer.at[j], sem_att.at[j])
        fold(j, 1, att_peer[j])

    def far_rows(j, slot):
        at = slice(slot * rows, (slot + 1) * rows)
        value = pred[j, 1, at, :] + jnp.dot(
            xs[yo, 2 + slot], w_all[j, yo].reshape(depth, chunk), preferred_element_type=F32
        )
        pred[j, 1, at, :] = value
        part_send(j, 2 + slot, value)

    attend(0)
    attend(2)
    push(att_half.at[pc, 0], att_peer.at[0], sem_att.at[0], mate, 2)

    @pl.when(mid == 1)
    def _():
        near_rows()
        for k in range(3):
            forward(1, k, 1)

    fold_first(0)
    x_relay(yo)
    pl.when(mid == 0)(functools.partial(forward, 1, 1, 0))
    fold_second(0)
    far_rows(0, 0)
    x_arrive(yo, 3)
    far_rows(0, 1)
    pl.when(mid == 0)(functools.partial(forward, 1, 2, 0))
    attend(1)
    attend(3)
    push(att_half.at[pc, 1], att_peer.at[1], sem_att.at[1], mate, 2)
    pred[1, 0] = product(1, y, 0)
    pred[1, 1] = product(1, y, 2)
    turn(yo, 2)
    turn(yo, 3)
    arrive(inv_row.at[2:4], sem_inv.at[1])
    spread(2)
    spread(3)
    fold_first(1)
    fold_second(1)
    far_rows(1, 0)
    far_rows(1, 1)

    def scale_rows(j, slot):
        arrive(p_in.at[j, slot], sem_p.at[j, slot])
        at = slice((slot % 2) * rows, (slot % 2 + 1) * rows)
        factor = inv[slot]
        raw = pred[j, slot // 2, at, :] + p_in[j, slot].astype(F32)
        s_all[j, slot] = (raw * factor * (factor * token_total ** (-0.5))).astype(BF16)

    def grad(j, at_y):
        return jnp.dot(
            xt[at_y], s_all[j].reshape(4 * rows, chunk), preferred_element_type=F32
        ).reshape(2, 4, piece, chunk)

    order = (3, 2, 1, 0)
    for j in range(2):
        for slot in (2, 3, 0, 1):
            scale_rows(j, slot)
        for near in range(2):
            first = 2 * ((z // 2 + 1 + near) % 2)
            for part in range(2):
                lead = pl.multiple_of((part * 4 + first) * piece, 16)
                s_y[j, part, pl.ds(first, 2)] = jnp.dot(
                    xt[yo, pl.ds(lead, 2 * piece), :], s_all[j].reshape(4 * rows, chunk),
                    preferred_element_type=F32,
                ).astype(BF16).reshape(2, piece, chunk)
            if j == 0:
                at = (j, slice(None), pl.ds(first, 2))
                push(s_y.at[at], r_y.at[at], sem_ry.at[j, near], yn_dev, 4)
            else:
                for r in ((3, 2), (1, 0))[near]:
                    at = (j, slice(None), zs[r])
                    push(s_y.at[at], r_y.at[at], sem_ry.at[j, r], yn_dev, 4)
        grad_f[j] = grad(j, y)

    def column_sum(j, part, g):
        return grad_f[j, part, g] + r_y[j, part, g].astype(F32)

    def z_push(j, part, g, dev):
        push(s_z.at[j, part, g], r_z.at[j, z, c], sem_rz.at[j], dev, 4)

    for j in range(2):
        for r in order:
            g = zs[r]
            if j == 1:
                arrive(r_y.at[j, :, g], sem_ry.at[j, r])
            elif r % 2:
                first = 2 * ((z // 2 + 1 + (3 - r) // 2) % 2)
                arrive(r_y.at[j, :, pl.ds(first, 2)], sem_ry.at[j, (3 - r) // 2])
            if r:
                for part in range(2):
                    s_z[j, part, g] = column_sum(j, part, g).astype(BF16)
                z_push(j, c, g, z_dev[r])
                z_push(j, pc, g, z_mate[r])
        for part in range(2):
            grad_f[j, part, z] = column_sum(j, part, z)
        s_z[j, pc, z] = grad_f[j, pc, z].astype(BF16)
        z_push(j, pc, z, mate)
    for j in range(2):
        amount(7 * piece, sem_rz.at[j]).wait()
        total = grad_f[j, c, z]
        for r in range(1, 4):
            total = total + r_z[j, zs[r], c].astype(F32)
        out_ref[:, cols(c, j)] = total
        total = jnp.zeros((piece, chunk), F32)
        for r in (3, 2, 1, 0):
            total = total + r_z[j, zs[r], pc].astype(F32)
        out_ref[:, cols(pc, j)] = total
    for group in range(5):
        amount(sent[group], send.at[group]).wait()
    pl.when(mid == 1)(amount(sum(relayed), send.at[5]).wait)


def put_kernel(att_ref, grad_ref, att_out, grad_out, sem):
    copies = [
        pltpu.make_async_copy(att_ref, att_out, sem.at[0]),
        pltpu.make_async_copy(grad_ref, grad_out, sem.at[1]),
    ]
    for copy in copies:
        copy.start()
    for copy in copies:
        copy.wait()


def local_fused(student_in, weight, queries, keys, values, lengths, assignment):
    rows, width = student_in.shape
    piece, features = weight.shape
    chunk = features // 4
    depth = width // 4
    token_total = rows * lax.axis_size("dp") * lax.axis_size("seq")
    vmem = pl.BlockSpec(memory_space=pltpu.VMEM)
    hbm = pl.BlockSpec(memory_space=pltpu.HBM)
    dma = pltpu.SemaphoreType.DMA
    quarter = (2, 4, piece, chunk)
    held = pl.pallas_call(
        functools.partial(fused_kernel, token_total),
        out_shape=(
            pltpu.VMEM((rows, features), BF16),
            pltpu.VMEM((piece, features), F32),
        ),
        in_specs=[hbm] * 7,
        out_specs=(vmem, vmem),
        scratch_shapes=[
            pltpu.VMEM((2, 4, rows, depth), BF16),
            pltpu.VMEM((2, rows, depth), BF16),
            pltpu.VMEM((2, depth, 4 * rows), BF16),
            pltpu.VMEM((2, 2) + quarter, BF16),
            pltpu.VMEM((2, piece, chunk), BF16),
            pltpu.VMEM((rows, features), BF16),
            pltpu.VMEM((2, 4, rows, HD), BF16),
            pltpu.SMEM(lengths.shape, jnp.int32),
            pltpu.SMEM(assignment.shape, jnp.int32),
            pltpu.VMEM((4, rows, 128), F32),
            pltpu.VMEM((4, 8, 128), F32),
            pltpu.VMEM((2, 2, 2 * rows, chunk), F32),
            pltpu.VMEM((2, 4, rows, chunk), BF16),
            pltpu.VMEM((2, 4, rows, chunk), BF16),
            pltpu.VMEM((2, 4, rows, chunk), BF16),
            pltpu.VMEM((2, 2, rows, chunk), BF16),
            pltpu.VMEM((2, rows, chunk), BF16),
            pltpu.VMEM((2,) + quarter, F32),
            pltpu.VMEM((2,) + quarter, BF16),
            pltpu.VMEM((2,) + quarter, BF16),
            pltpu.VMEM((2,) + quarter, BF16),
            pltpu.VMEM((2, 4, 2, piece, chunk), BF16),
            pltpu.VMEM((8192, 128), BF16),
            dma((9,)),
            dma((6,)),
            dma((2, 4)),
            dma((2,)),
            dma((4,)),
            dma((2, 3)),
            dma((2,)),
            dma((2,)),
            dma((2, 4)),
            dma((2, 4)),
            dma((2,)),
        ],
        compiler_params=pltpu.CompilerParams(collective_id=0, has_side_effects=True),
        name="distill",
    )(student_in, weight, queries, keys, values, lengths, assignment)
    return pl.pallas_call(
        put_kernel,
        out_shape=(
            jax.ShapeDtypeStruct((rows, features), BF16),
            jax.ShapeDtypeStruct((piece, features), F32),
        ),
        in_specs=[vmem] * 2,
        out_specs=(hbm, hbm),
        scratch_shapes=[dma((2,))],
        name="put",
    )(*(pltpu.with_memory_space_constraint(h, pltpu.VMEM) for h in held))


def fits(student_in, weight, queries, keys, values, lengths, assignment):
    rows, width = student_in.shape
    piece, features = weight.shape
    return (
        lax.axis_size("dp") == 8
        and lax.axis_size("seq") == 4
        and rows == BLK
        and assignment.shape[1] == 4
        and piece % 16 == 0
        and width == 32 * piece
        and width % 512 == 0
        and features == HQ * HD
        and keys.shape[1] == HD
    )


def dispatch(*arrays):
    return local_fused(*arrays) if fits(*arrays) else local(*arrays)


def solution(mesh):
    placed = (
        P(("dp", "seq"), None),
        P(("dp", "seq"), None),
        P(("dp", "seq"), None),
        P(("dp", "seq"), None),
        P(("dp", "seq"), None),
        P("dp", None),
        P("dp", None),
    )
    return jax.shard_map(
        dispatch,
        mesh=mesh,
        in_specs=placed,
        out_specs=(P(("dp", "seq"), None), P(("dp", "seq"), None)),
        check_vma=False,
    )
```

```python
import functools
import math

import jax
import jax.numpy as jnp
from jax import lax
from jax.experimental import pallas as pl
from jax.experimental.pallas import tpu as pltpu
from jax.sharding import PartitionSpec as P

HD = 128
HQ = 4
BLK = 128


EPSILON = 1e-06
NEGATIVE = -1e30


def locate(assign_row, doc_ends, first_slot, count):
    slot_ids = first_slot + jnp.arange(count, dtype=jnp.int32)
    block_ids = slot_ids // BLK
    block_table = jnp.arange(assign_row.shape[0], dtype=jnp.int32)
    placed = jnp.sum(
        jnp.where(block_ids[:, None] == block_table[None, :], assign_row[None, :], 0), axis=1
    )
    position = placed * BLK + slot_ids % BLK
    document = jnp.sum((position[:, None] >= doc_ends[None, :]).astype(jnp.int32), axis=1)
    return (position, document)


def absorb_block(state, key_block, value_block, query_heads, allowed):
    run_max, run_total, run_acc = state
    scores = jnp.einsum(
        "qhd,kd->hqk", query_heads, key_block, preferred_element_type=jnp.float32
    ) * HD ** (-0.5)
    masked = jnp.where(allowed[None], scores, NEGATIVE)
    new_max = jnp.maximum(run_max, jnp.max(masked, axis=-1))
    fading = jnp.exp(run_max - new_max)
    exp_terms = jnp.where(allowed[None], jnp.exp(masked - new_max[:, :, None]), 0.0)
    new_total = run_total * fading + jnp.sum(exp_terms, axis=-1)
    mixture = jnp.einsum(
        "hqk,kd->qhd",
        exp_terms.astype(jnp.bfloat16),
        value_block,
        preferred_element_type=jnp.float32,
    )
    new_acc = run_acc * fading.T[:, :, None] + mixture
    return (new_max, new_total, new_acc)


def local(student_in, weight, queries, keys, values, lengths, assignment):
    rows = queries.shape[0]
    assign_row = assignment[0]
    doc_ends = jnp.cumsum(lengths[0])
    query_pos, query_doc = locate(assign_row, doc_ends, lax.axis_index("seq") * rows, rows)
    query_heads = queries.reshape(rows, HQ, HD)
    start_state = (
        jnp.full((HQ, rows), NEGATIVE, jnp.float32),
        jnp.zeros((HQ, rows), jnp.float32),
        jnp.zeros((rows, HQ, HD), jnp.float32),
    )
    key_piece = lax.all_gather(keys, "seq", axis=0, tiled=True)
    value_piece = lax.all_gather(values, "seq", axis=0, tiled=True)
    count = key_piece.shape[0]
    step_rows = math.gcd(count, 512)
    steps_count = count // step_rows
    key_pos, key_doc = locate(assign_row, doc_ends, jnp.int32(0), count)

    def one_step(running, slabs):
        key_block, value_block, key_position, key_document = slabs
        allowed = (query_doc[:, None] == key_document[None, :]) & (
            query_pos[:, None] >= key_position[None, :]
        )
        updated = absorb_block(running, key_block, value_block, query_heads, allowed)
        return (updated, None)

    slabs = (
        key_piece.reshape(steps_count, step_rows, HD),
        value_piece.reshape(steps_count, step_rows, HD),
        key_pos.reshape(steps_count, step_rows),
        key_doc.reshape(steps_count, step_rows),
    )
    result, _ = lax.scan(one_step, start_state, slabs)
    final_max, final_total, final_acc = result
    attention = (final_acc / final_total.T[:, :, None]).reshape(rows, HQ * HD).astype(jnp.bfloat16)
    as_float = student_in.astype(jnp.float32)
    normed = (
        as_float * lax.rsqrt(jnp.mean(as_float * as_float, axis=1, keepdims=True) + EPSILON)
    ).astype(jnp.bfloat16)
    group_rows = lax.all_gather(weight, "seq", axis=0, tiled=True)
    columns = normed
    predicted = jnp.dot(
        columns,
        lax.all_gather(group_rows, "dp", axis=0, tiled=True),
        preferred_element_type=jnp.float32,
    )
    dp_count = lax.axis_size("dp")
    seq_count = lax.axis_size("seq")
    token_total = rows * dp_count * seq_count
    scaled = ((predicted - attention.astype(jnp.float32)) * token_total ** (-0.5)).astype(
        jnp.bfloat16
    )
    columns = normed
    outer_rows = lax.psum_scatter(
        lax.dot_general(
            columns, scaled, (((0,), (0,)), ((), ())), preferred_element_type=jnp.float32
        ).astype(jnp.bfloat16),
        "dp",
        scatter_dimension=0,
        tiled=True,
    )
    weight_grad = lax.psum_scatter(outer_rows, "seq", scatter_dimension=0, tiled=True).astype(
        jnp.float32
    )
    return (attention, weight_grad)


MESH = pl.DeviceIdType.MESH
F32 = jnp.float32
BF16 = jnp.bfloat16


def fused_kernel(
    token_total,
    x_hbm, w_hbm, q_hbm, k_hbm, v_hbm, len_hbm, asg_hbm,
    att_ref, out_ref,
    xs, xo, xt, w_all, w_peer, q_ref, kv_all, len_ref, asg_ref, inv, inv_row, pred, p_out, p_in,
    s_all, att_half, att_peer, grad_f, s_y, r_y, s_z, r_z, bulk,
    local_sem, send, sem_w, sem_w_far, sem_kv, sem_x, sem_inv, sem_att, sem_p, sem_ry, sem_rz,
):
    rows = q_ref.shape[0]
    piece = w_hbm.shape[0]
    half = w_hbm.shape[1] // 2
    chunk = half // 2
    depth = xs.shape[3]
    dp, z = lax.axis_index("dp"), lax.axis_index("seq")
    c = dp % 2
    pc = 1 - c
    x = (dp // 2) % 2
    y = dp // 4
    yo = 1 - y
    dp_m = dp + 1 - 2 * c
    mate = (dp_m, z)
    xn_dev = (dp + 2 - 4 * x, z)
    xn_mate = (dp_m + 2 - 4 * x, z)
    yn_dev = (dp + 4 - 8 * y, z)
    yn_mate = (dp_m + 4 - 8 * y, z)
    zs = (z, z + 1 - 2 * (z % 2), z + 2 - 4 * (z // 2), 3 - z)
    mid = ((z + 1) // 2) % 2
    z_two = mid * zs[3] + (1 - mid) * zs[2]
    z_from = (
        mid * zs[3] + (1 - mid) * zs[1],
        zs[2],
        mid * zs[1] + (1 - mid) * zs[3],
    )
    z_dev = [(dp, zs[r]) for r in range(4)]
    z_mate = [(dp_m, zs[r]) for r in range(4)]

    def cols(core, j):
        return pl.ds(pl.multiple_of(core * half + j * chunk, 128), chunk)

    def width(at_y, at_x):
        return pl.ds(pl.multiple_of((at_y * 2 + at_x) * depth, 128), depth)

    barrier = pltpu.get_barrier_semaphore()
    greeted = [mate, xn_dev, xn_mate, yn_dev, yn_mate] + z_dev[1:] + z_mate[1:]
    for dev in greeted:
        pl.semaphore_signal(barrier, inc=1, device_id=dev, device_id_type=MESH)

    def lines(ref):
        return math.prod(ref.shape) * jnp.dtype(ref.dtype).itemsize // 256

    def fetch(at, *pairs):
        copies = [pltpu.make_async_copy(a, b, local_sem.at[at]) for a, b in pairs]
        for copy in copies:
            copy.start()
        return sum(lines(b) for _, b in pairs)

    def amount(count, sem):
        part = bulk.at[pl.ds(0, count)]
        return pltpu.make_async_copy(part, part, sem)

    get_w = [
        fetch(
            j,
            (w_hbm.at[:, cols(c, j)], w_all.at[j, y, c, z]),
            (w_hbm.at[:, cols(pc, j)], w_peer.at[j]),
        )
        for j in range(2)
    ]
    get_xo = [
        fetch(1, (x_hbm.at[:, width(at, 1 - x)], xo.at[at])) for i, at in enumerate((y, yo))
    ]
    get_kv = fetch(1, *((ref, kv_all.at[i, z]) for i, ref in enumerate((k_hbm, v_hbm))))
    get_xs = fetch(1, *((x_hbm.at[:, width(at, x)], xs.at[at, 0]) for at in (y, yo)))
    get_q = fetch(1, (q_hbm, q_ref))
    fetch(2, (len_hbm, len_ref))
    fetch(3, (asg_hbm, asg_ref))
    pl.semaphore_wait(barrier, len(greeted))

    sent = [0, 0, 0]

    def push(src, dst, rsem, dev, group, counted=True):
        copy = pltpu.make_async_remote_copy(
            src_ref=src, dst_ref=dst, send_sem=send.at[(0, 1, 1, 0, 2)[group]], recv_sem=rsem,
            device_id=dev, device_id_type=MESH,
        )
        copy.start()
        if counted:
            sent[(0, 1, 1, 0, 2)[group]] += lines(src)

    def arrive(dst, rsem):
        pltpu.make_async_remote_copy(
            src_ref=dst, dst_ref=dst, send_sem=send.at[0], recv_sem=rsem,
            device_id=mate, device_id_type=MESH,
        ).wait_recv()

    def w_along(j, to):
        dst, sem = w_all.at[j, y, c, z], sem_w.at[j, z]
        push(dst, dst, sem, (dp, to), 0)
        push(w_peer.at[j], dst, sem, (dp_m, to), 0)

    def w_across(j):
        dst, sem = w_all.at[j, y, c, z], sem_w.at[j, z]
        push(dst, dst, sem_w_far.at[j], yn_dev, 0)
        push(w_peer.at[j], dst, sem_w_far.at[j], yn_mate, 0)
        push(w_peer.at[j], dst, sem, mate, 0)

    kv_own = kv_all.at[:, z]
    amount(get_w[0], local_sem.at[0]).wait()
    w_along(0, z_two)
    w_along(0, zs[1])
    w_across(0)
    amount(get_w[1] + sum(get_xo) + get_kv + get_xs + get_q, local_sem.at[1]).wait()
    push(kv_own, kv_own, sem_kv.at[z], (dp, z_two), 2)
    push(kv_own, kv_own, sem_kv.at[z], z_dev[1], 2)
    for at_y in (y, yo):
        push(xo.at[at_y], xs.at[at_y, 2], sem_x.at[2 * at_y], xn_dev, 1)
    w_along(1, z_two)
    w_along(1, zs[1])
    w_across(1)
    push(xs.at[:, 0], xs.at[:, 1], sem_x.at[4], mate, 1)

    step = 16

    @pl.loop(0, rows // step)
    def _(i):
        at = pl.ds(pl.multiple_of(i * step, step), step)
        total = jnp.zeros((step, 1), F32)
        for ref in (xs.at[0, 0], xs.at[1, 0], xo.at[0], xo.at[1]):
            block = ref[at, :].astype(F32)
            total = total + jnp.sum(block * block, axis=1, keepdims=True)
        factor = lax.rsqrt(total / (4 * depth) + EPSILON)
        inv[0, at, :] = jnp.broadcast_to(factor, (step, 128))

    inv_row[0] = inv[0].T[:8]
    push(inv_row.at[0], inv_row.at[1], sem_inv.at[0], mate, 2)
    push(inv_row.at[0], inv_row.at[2], sem_inv.at[1], xn_dev, 2)
    push(inv_row.at[0], inv_row.at[3], sem_inv.at[1], xn_mate, 2)

    relayed = []

    def relay(ref, sem, k, where):
        if k == 2 or where == 0:
            return
        copy = pltpu.make_async_remote_copy(
            src_ref=ref, dst_ref=ref, send_sem=send.at[3], recv_sem=sem,
            device_id=z_dev[1], device_id_type=MESH,
        )
        if where == 1:
            copy.start()
        else:
            pl.when(mid == 1)(copy.start)
        relayed.append(lines(ref))

    def forward(j, k, where=None):
        at = w_all.at[j, y, :, z_from[k]]
        arrive(at, sem_w.at[j, z_from[k]])
        relay(at, sem_w.at[j, z_from[k]], k, where)
        push(at, at, sem_w_far.at[j], yn_dev, 3, where != 1)

    def kv_forward(k, where):
        at = kv_all.at[:, z_from[k]]
        arrive(at, sem_kv.at[z_from[k]])
        relay(at, sem_kv.at[z_from[k]], k, where)

    def x_arrive(at_y, slot):
        arrive(xs.at[at_y, slot], sem_x.at[2 * at_y + slot - 2])

    def x_relay(at_y):
        x_arrive(at_y, 2)
        push(xs.at[at_y, 2], xs.at[at_y, 3], sem_x.at[2 * at_y + 1], mate, 2)

    def turn(at_y, slot):
        for j in range(depth // 128):
            at = slice(j * 128, (j + 1) * 128)
            xt[at_y, at, slot * rows : (slot + 1) * rows] = xs[at_y, slot, :, at].T

    def product(j, at_y, first):
        return jnp.dot(
            xs[at_y, first : first + 2].reshape(2 * rows, depth),
            w_all[j, at_y].reshape(depth, chunk),
            preferred_element_type=F32,
        )

    arrive(xs.at[:, 1], sem_x.at[4])
    for slot in range(2):

        @pl.loop(0, 2)
        def _(at_y):
            turn(at_y, slot)

    def spread(slot):
        inv[slot] = jnp.broadcast_to(inv_row[slot, :1], (rows, 128)).T

    for k in range(3):
        forward(0, k)
    for j in range(2):
        arrive(w_all.at[j, y, pc, z], sem_w.at[j, z])
    pred[0, 0] = product(0, y, 0)

    @pl.when(mid == 1)
    def _():
        for k in range(3):
            kv_forward(k, 1)

    x_relay(y)
    arrive(inv_row.at[1], sem_inv.at[0])
    spread(1)
    pltpu.make_async_copy(len_hbm, len_ref, local_sem.at[2]).wait()
    pltpu.make_async_copy(asg_hbm, asg_ref, local_sem.at[3]).wait()

    def near_rows():
        turn(y, 2)
        x_arrive(y, 3)
        turn(y, 3)
        pred[0, 1] = product(0, y, 2)

    @pl.when(mid == 0)
    def _():
        near_rows()
        forward(1, 0, 0)
        for k in range(3):
            kv_forward(k, 0)

    ends = []
    total = 0
    for i in range(len_ref.shape[1]):
        total = total + len_ref[0, i]
        ends.append(total)

    def document(position):
        found = jnp.zeros(position.shape, jnp.int32)
        for end in ends:
            found = found + (position >= end).astype(jnp.int32)
        return found

    lanes = lax.broadcasted_iota(jnp.int32, (1, BLK), 1)
    k_pos = jnp.concatenate([asg_ref[0, j] * BLK + lanes for j in range(4)], axis=1)
    q_pos = asg_ref[0, z] * BLK + lax.broadcasted_iota(jnp.int32, (rows, 1), 0)
    allowed = (document(q_pos) == document(k_pos)) & (q_pos >= k_pos)

    def attend(h):
        k_all = kv_all[0].reshape(4 * rows, HD)
        v_all = kv_all[1].reshape(4 * rows, HD)
        scores = lax.dot_general(
            q_ref[:, h * HD : (h + 1) * HD], k_all, (((1,), (1,)), ((), ())),
            preferred_element_type=F32,
        ) * HD ** (-0.5)
        masked = jnp.where(allowed, scores, NEGATIVE)
        top = jnp.max(masked, axis=1, keepdims=True)
        terms = jnp.where(allowed, jnp.exp(masked - top), 0.0)
        totals = jnp.sum(terms, axis=1, keepdims=True)
        mixture = jnp.dot(terms.astype(BF16), v_all, preferred_element_type=F32)
        done = (mixture / totals).astype(BF16)
        att_ref[:, h * HD : (h + 1) * HD] = done
        att_half[h // 2, h % 2] = done

    def part_send(j, slot, value):
        p_out[j, slot] = value.astype(BF16)
        at = (j, (slot + 2) % 4)
        push(p_out.at[j, slot], p_in.at[at], sem_p.at[j * (1 + at[1])], xn_dev, 2)

    def fold(j, slot, attended):
        at = slice(slot * rows, (slot + 1) * rows)
        value = pred[j, 0, at, :] - attended.astype(F32) / inv[slot]
        pred[j, 0, at, :] = value
        part_send(j, slot, value)

    def fold_first(j):
        arrive(w_all.at[j, yo], sem_w_far.at[j])
        pred[j, 0] += product(j, yo, 0)
        fold(j, 0, att_half[c, j])

    def fold_second(j):
        arrive(att_peer.at[j], sem_att.at[j])
        fold(j, 1, att_peer[j])

    def far_rows(j, slot):
        at = slice(slot * rows, (slot + 1) * rows)
        value = pred[j, 1, at, :] + jnp.dot(
            xs[yo, 2 + slot], w_all[j, yo].reshape(depth, chunk), preferred_element_type=F32
        )
        pred[j, 1, at, :] = value
        part_send(j, 2 + slot, value)

    attend(0)
    attend(2)
    push(att_half.at[pc, 0], att_peer.at[0], sem_att.at[0], mate, 2)

    @pl.when(mid == 1)
    def _():
        near_rows()
        for k in range(3):
            forward(1, k, 1)

    fold_first(0)
    x_relay(yo)
    pl.when(mid == 0)(functools.partial(forward, 1, 1, 0))
    fold_second(0)
    far_rows(0, 0)
    x_arrive(yo, 3)
    far_rows(0, 1)
    pl.when(mid == 0)(functools.partial(forward, 1, 2, 0))
    attend(1)
    attend(3)
    push(att_half.at[pc, 1], att_peer.at[1], sem_att.at[1], mate, 2)
    pred[1, 0] = product(1, y, 0)
    pred[1, 1] = product(1, y, 2)
    turn(yo, 2)
    turn(yo, 3)
    arrive(inv_row.at[2:4], sem_inv.at[1])
    spread(2)
    spread(3)
    fold_first(1)
    fold_second(1)
    far_rows(1, 0)
    far_rows(1, 1)

    def scale_rows(j, slot):
        if j == 1:
            arrive(p_in.at[j, slot], sem_p.at[1 + slot])
        elif slot == 2:
            arrive(p_in.at[j], sem_p.at[0])
        at = slice((slot % 2) * rows, (slot % 2 + 1) * rows)
        factor = inv[slot]
        raw = pred[j, slot // 2, at, :] + p_in[j, slot].astype(F32)
        s_all[j, slot] = (raw * factor * (factor * token_total ** (-0.5))).astype(BF16)

    def grad(j, at_y):
        return jnp.dot(
            xt[at_y], s_all[j].reshape(4 * rows, chunk), preferred_element_type=F32
        ).reshape(2, 4, piece, chunk)

    order = (3, 2, 1, 0)
    for j in range(2):
        for slot in (2, 3, 0, 1):
            scale_rows(j, slot)
        for near in range(2):
            first = 2 * ((z // 2 + 1 + near) % 2)
            for part in range(2):
                lead = pl.multiple_of((part * 4 + first) * piece, 16)
                s_y[j, part, pl.ds(first, 2)] = jnp.dot(
                    xt[yo, pl.ds(lead, 2 * piece), :], s_all[j].reshape(4 * rows, chunk),
                    preferred_element_type=F32,
                ).astype(BF16).reshape(2, piece, chunk)
            if j == 0:
                at = (j, slice(None), pl.ds(first, 2))
                push(s_y.at[at], r_y.at[at], sem_ry.at[near], yn_dev, 4)
            else:
                for r in ((3, 2), (1, 0))[near]:
                    at = (j, slice(None), zs[r])
                    push(s_y.at[at], r_y.at[at], sem_ry.at[2 + r], yn_dev, 4)
        grad_f[j] = grad(j, y)

    def column_sum(j, part, g):
        return grad_f[j, part, g] + r_y[j, part, g].astype(F32)

    def z_push(j, part, g, dev):
        push(s_z.at[j, part, g], r_z.at[j, z, c], sem_rz.at[j], dev, 4)

    for j in range(2):
        for r in order:
            g = zs[r]
            if j == 1:
                arrive(r_y.at[j, :, g], sem_ry.at[2 + r])
            elif r % 2:
                first = 2 * ((z // 2 + 1 + (3 - r) // 2) % 2)
                arrive(r_y.at[j, :, pl.ds(first, 2)], sem_ry.at[(3 - r) // 2])
            if r:
                for part in range(2):
                    s_z[j, part, g] = column_sum(j, part, g).astype(BF16)
                z_push(j, c, g, z_dev[r])
                z_push(j, pc, g, z_mate[r])
        for part in range(2):
            grad_f[j, part, z] = column_sum(j, part, z)
        s_z[j, pc, z] = grad_f[j, pc, z].astype(BF16)
        z_push(j, pc, z, mate)
    for j in range(2):
        amount(7 * piece, sem_rz.at[j]).wait()
        total = grad_f[j, c, z]
        for r in range(1, 4):
            total = total + r_z[j, zs[r], c].astype(F32)
        out_ref[:, cols(c, j)] = total
        total = jnp.zeros((piece, chunk), F32)
        for r in (3, 2, 1, 0):
            total = total + r_z[j, zs[r], pc].astype(F32)
        out_ref[:, cols(pc, j)] = total
    for group in range(3):
        amount(sent[group], send.at[group]).wait()
    pl.when(mid == 1)(amount(sum(relayed), send.at[3]).wait)


def put_kernel(att_ref, grad_ref, att_out, grad_out, sem):
    copies = [
        pltpu.make_async_copy(att_ref, att_out, sem.at[0]),
        pltpu.make_async_copy(grad_ref, grad_out, sem.at[1]),
    ]
    for copy in copies:
        copy.start()
    for copy in copies:
        copy.wait()


def local_fused(student_in, weight, queries, keys, values, lengths, assignment):
    rows, width = student_in.shape
    piece, features = weight.shape
    chunk = features // 4
    depth = width // 4
    token_total = rows * lax.axis_size("dp") * lax.axis_size("seq")
    vmem = pl.BlockSpec(memory_space=pltpu.VMEM)
    hbm = pl.BlockSpec(memory_space=pltpu.HBM)
    dma = pltpu.SemaphoreType.DMA
    quarter = (2, 4, piece, chunk)
    held = pl.pallas_call(
        functools.partial(fused_kernel, token_total),
        out_shape=(
            pltpu.VMEM((rows, features), BF16),
            pltpu.VMEM((piece, features), F32),
        ),
        in_specs=[hbm] * 7,
        out_specs=(vmem, vmem),
        scratch_shapes=[
            pltpu.VMEM((2, 4, rows, depth), BF16),
            pltpu.VMEM((2, rows, depth), BF16),
            pltpu.VMEM((2, depth, 4 * rows), BF16),
            pltpu.VMEM((2, 2) + quarter, BF16),
            pltpu.VMEM((2, piece, chunk), BF16),
            pltpu.VMEM((rows, features), BF16),
            pltpu.VMEM((2, 4, rows, HD), BF16),
            pltpu.SMEM(lengths.shape, jnp.int32),
            pltpu.SMEM(assignment.shape, jnp.int32),
            pltpu.VMEM((4, rows, 128), F32),
            pltpu.VMEM((4, 8, 128), F32),
            pltpu.VMEM((2, 2, 2 * rows, chunk), F32),
            pltpu.VMEM((2, 4, rows, chunk), BF16),
            pltpu.VMEM((2, 4, rows, chunk), BF16),
            pltpu.VMEM((2, 4, rows, chunk), BF16),
            pltpu.VMEM((2, 2, rows, chunk), BF16),
            pltpu.VMEM((2, rows, chunk), BF16),
            pltpu.VMEM((2,) + quarter, F32),
            pltpu.VMEM((2,) + quarter, BF16),
            pltpu.VMEM((2,) + quarter, BF16),
            pltpu.VMEM((2,) + quarter, BF16),
            pltpu.VMEM((2, 4, 2, piece, chunk), BF16),
            pltpu.VMEM((8192, 128), BF16),
            dma((4,)),
            dma((4,)),
            dma((2, 4)),
            dma((2,)),
            dma((4,)),
            dma((5,)),
            dma((2,)),
            dma((2,)),
            dma((5,)),
            dma((6,)),
            dma((2,)),
        ],
        compiler_params=pltpu.CompilerParams(collective_id=0, has_side_effects=True),
        name="distill",
    )(student_in, weight, queries, keys, values, lengths, assignment)
    return pl.pallas_call(
        put_kernel,
        out_shape=(
            jax.ShapeDtypeStruct((rows, features), BF16),
            jax.ShapeDtypeStruct((piece, features), F32),
        ),
        in_specs=[vmem] * 2,
        out_specs=(hbm, hbm),
        scratch_shapes=[dma((2,))],
        name="put",
    )(*(pltpu.with_memory_space_constraint(h, pltpu.VMEM) for h in held))


def fits(student_in, weight, queries, keys, values, lengths, assignment):
    rows, width = student_in.shape
    piece, features = weight.shape
    return (
        lax.axis_size("dp") == 8
        and lax.axis_size("seq") == 4
        and rows == BLK
        and assignment.shape[1] == 4
        and piece % 16 == 0
        and width == 32 * piece
        and width % 512 == 0
        and features == HQ * HD
        and keys.shape[1] == HD
    )


def dispatch(*arrays):
    return local_fused(*arrays) if fits(*arrays) else local(*arrays)


def solution(mesh):
    placed = (
        P(("dp", "seq"), None),
        P(("dp", "seq"), None),
        P(("dp", "seq"), None),
        P(("dp", "seq"), None),
        P(("dp", "seq"), None),
        P("dp", None),
        P("dp", None),
    )
    return jax.shard_map(
        dispatch,
        mesh=mesh,
        in_specs=placed,
        out_specs=(P(("dp", "seq"), None), P(("dp", "seq"), None)),
        check_vma=False,
    )
```
